32 devices in a mesh: data: 1 (over z), store: 4 (over y), model: 8 (over x, core).
Axes of the slice: x: 4, y: 4, z: 1, core: 2. Of those that a mesh axis runs over, the one named last changes fastest.
The devices are a block of a 4x4x8 slice.
Arguments:
- queries: bfloat16 [256, 2048], P('data')
- w_head: bfloat16 [2048, 32000], P(None, 'model')
- store_keys: bfloat16 [262144, 2048], P(('store', 'model'))
- store_tok: int32 [262144], P(('store', 'model'))
- temperature: float32 [], replicated
- mix_weight: float32 [], replicated
Outputs:
- output: float32 [256, 32000], P(('data', 'store'), 'model')
All inputs are finite; a program needn't handle non-finite values.
Results may differ from the reference program's by a relative error of at most 0.001.
Values are sent between devices in bfloat16 or wider.
A program may use at most 768 MiB of HBM per device.

```python
import jax
import jax.numpy as jnp
from jax import lax

HIDDEN = 2048
VOCAB = 32000
ROWS_DEV = 64
KEYS_DEV = 8192
STORE_DEVS = 4
MODEL_DEVS = 8
BATCH = ROWS_DEV * STORE_DEVS
SHARDS = STORE_DEVS * MODEL_DEVS
N_KEYS = KEYS_DEV * SHARDS


def setup_inputs(seed: int = 0, part: int = 0) -> dict:
    base_key = jax.random.key(seed)
    part_key = jax.random.fold_in(base_key, part)
    key_head, key_store, key_tok_a, key_tok_b, key_temp, key_mix = jax.random.split(base_key, 6)
    queries = jax.random.normal(part_key, (BATCH, HIDDEN), jnp.float32)
    w_head = jax.random.normal(key_head, (HIDDEN, VOCAB), jnp.float32) * HIDDEN ** -0.5
    store_keys = jax.random.normal(key_store, (N_KEYS, HIDDEN), jnp.float32)
    tok_a = jax.random.randint(key_tok_a, (N_KEYS,), 0, VOCAB, jnp.int32)
    tok_b = jax.random.randint(key_tok_b, (N_KEYS,), 0, VOCAB, jnp.int32)
    store_tok = jnp.minimum(tok_a, tok_b).at[0].set(0).at[N_KEYS - 1].set(VOCAB - 1)
    temperature = (6.0 * HIDDEN) ** 0.5 / 1.5 * jax.random.uniform(key_temp, (), jnp.float32, minval=0.6, maxval=1.5)
    mix_weight = jax.random.uniform(key_mix, (), jnp.float32, minval=0.25, maxval=0.5)
    return {"queries": queries.astype(jnp.bfloat16), "w_head": w_head.astype(jnp.bfloat16), "store_keys": store_keys.astype(jnp.bfloat16), "store_tok": store_tok, "temperature": temperature, "mix_weight": mix_weight}


def reference(queries, w_head, store_keys, store_tok, temperature, mix_weight):
    key_blocks = store_keys.reshape(SHARDS, KEYS_DEV, HIDDEN)
    tok_blocks = store_tok.reshape(SHARDS, KEYS_DEV)

    def block_scores(block):
        key_dots = jnp.dot(block, queries.T, preferred_element_type=jnp.float32)
        key_norms = jnp.sum(jnp.square(block.astype(jnp.float32)), axis=1)
        return (2.0 * key_dots - key_norms[:, None]) / temperature

    block_top = lax.map(lambda block: jnp.max(block_scores(block), axis=0), key_blocks)
    row_top = jnp.max(block_top, axis=0)

    def accumulate(carry, pair):
        histogram, row_total = carry
        block, tok_ids = pair
        weights = jnp.exp(block_scores(block) - row_top)
        histogram = histogram + jax.ops.segment_sum(weights, tok_ids, num_segments=VOCAB)
        row_total = row_total + jnp.sum(weights, axis=0)
        return (histogram, row_total), None

    init_state = (jnp.zeros((VOCAB, BATCH), jnp.float32), jnp.zeros((BATCH,), jnp.float32))
    (histogram, row_total), _ = lax.scan(accumulate, init_state, (key_blocks, tok_blocks))
    knn_prob = (histogram / row_total).T
    logits = jnp.dot(queries, w_head, preferred_element_type=jnp.float32)
    lm_exp = jnp.exp(logits - jnp.max(logits, axis=1, keepdims=True))
    lm_prob = lm_exp / jnp.sum(lm_exp, axis=1, keepdims=True)
    return jnp.log(mix_weight * knn_prob + (1.0 - mix_weight) * lm_prob)
```

```python
import functools

import jax
import jax.numpy as jnp
from jax import lax
from jax.experimental import pallas as pl
from jax.experimental.pallas import tpu as pltpu
from jax.sharding import PartitionSpec as P

F32 = jnp.float32
BF16 = jnp.bfloat16
LANES = 128
BATCH = 4
MESH_ID = pl.DeviceIdType.MESH


def _scores_kernel(n_blocks, shards, tok_ref, rtau_ref, q_ref, k_ref, h_ref, stat_ref, hist, vals, top, stage, sem):
    step = pl.program_id(0)
    n_x, n_core, n_row, pairs, _ = shards
    block = k_ref.shape[0]
    rows = q_ref.shape[0]
    keys = vals.shape[0] // 2
    vocab = hist.shape[0] // 2

    zero_rows = hist.shape[0] // n_blocks
    zero_step = 64 if zero_rows % 64 == 0 else 8
    zero_base = step * zero_rows

    def clear(i, _):
        at = pl.multiple_of(zero_base + i * zero_step, 8)
        hist[pl.ds(at, zero_step), :] = jnp.zeros((zero_step, LANES), F32)
        return 0

    lax.fori_loop(0, zero_rows // zero_step, clear, 0)

    @pl.when(step == 0)
    def _():
        top[...] = jnp.full(top.shape, -jnp.inf, F32)

    sub = min(256, block)
    for part in range(block // sub):
        key = k_ref[part * sub : (part + 1) * sub, :]
        dots = lax.dot_general(key, q_ref[...], (((1,), (1,)), ((), ())), preferred_element_type=F32)
        wide = key.astype(F32)
        norms = jnp.sum(wide * wide, axis=1, keepdims=True)
        score = (2.0 * dots - norms) * rtau_ref[0]
        top[...] = jnp.maximum(top[...], jnp.max(score.reshape(sub // 8, 8, rows), axis=0))
        base = 2 * (step * block + part * sub)
        for half in range(2):
            vals[pl.ds(base + half, sub, stride=2), :] = score[:, half * LANES : (half + 1) * LANES]

    @pl.when(step == n_blocks - 1)
    def _():
        best = jnp.max(top[...], axis=0, keepdims=True)
        pair = jnp.concatenate([best[:, :LANES], best[:, LANES:]], axis=0)
        best8 = jnp.concatenate([pair] * 4, axis=0)

        def weigh(i, total):
            at = pl.multiple_of(i * 64, 64)
            old = vals[pl.ds(at, 64), :].reshape(8, 8, LANES)
            new = jnp.exp(old - best8[None])
            vals[pl.ds(at, 64), :] = new.reshape(64, LANES)
            return total + jnp.sum(new, axis=0)

        sum8 = lax.fori_loop(0, 2 * keys // 64, weigh, jnp.zeros((8, LANES), F32))
        total = sum8[0:2] + sum8[2:4] + sum8[4:6] + sum8[6:8]
        zeros6 = jnp.zeros((6, LANES), F32)
        stat_ref[...] = jnp.concatenate([pair, zeros6, total, zeros6], axis=0)

        per_trip = 4 * BATCH

        def scatter(i, _):
            first = i * per_trip
            for b in range(per_trip // BATCH):
                toks = [tok_ref[first + b * BATCH + j] for j in range(BATCH)]
                spots = [pl.ds(pl.multiple_of(2 * t, 2), 2) for t in toks]
                olds = [hist[p, :] for p in spots]
                news = []
                for j in range(BATCH):
                    base = olds[j]
                    for k in range(j):
                        base = jnp.where(toks[j] == toks[k], news[k], base)
                    at = pl.multiple_of(2 * (first + b * BATCH + j), 2)
                    news.append(base + vals[pl.ds(at, 2), :])
                for j in range(BATCH):
                    hist[spots[j], :] = news[j]
            return 0

        lax.fori_loop(0, keys // per_trip, scatter, 0)

        low = lax.broadcasted_iota(jnp.int32, (16, LANES), 1) < LANES // 2
        vocab_loc = 2 * pairs
        copies = []
        for owner in range(n_x * n_core):
            slot = owner % 2
            if owner >= 2:
                copies[owner - 2].wait()

            def pack(i, _, owner=owner, slot=slot):
                p = pl.multiple_of(i * 16, 16)
                for half in range(2):
                    a = hist[pl.ds(2 * (owner * vocab_loc + p) + half, 16, stride=2), :]
                    b = hist[pl.ds(2 * (owner * vocab_loc + pairs + p) + half, 16, stride=2), :]
                    stage[slot, 2 * half, pl.ds(p, 16), :] = jnp.where(low, a, pltpu.roll(b, 64, axis=1)).astype(BF16)
                    stage[slot, 2 * half + 1, pl.ds(p, 16), :] = jnp.where(low, pltpu.roll(a, 64, axis=1), b).astype(BF16)
                return 0

            lax.fori_loop(0, pairs // 16, pack, 0)
            copy = pltpu.make_async_copy(stage.at[slot], h_ref.at[owner // n_core, owner % n_core], sem.at[slot])
            copy.start()
            copies.append(copy)
        copies[-2].wait()
        copies[-1].wait()


def _exchange_kernel(ring, quarters, stat_ref, h_ref, out_ref, sout_ref,
                     own, par, ring1, ring2, fs, st_recv, st_buf,
                     own_sem, p_send, p_recv, r1_send, r1_recv, r2_send, r2_recv, st_send, st_rsem):
    s = lax.axis_index("store")
    m = lax.axis_index("model")
    x = lax.div(m, 2)
    c = lax.rem(m, 2)
    partner = {"store": s, "model": 2 * x + 1 - c}

    def along_y(d):
        return {"store": lax.rem(s + d + ring, ring), "model": m}

    def along_x(d):
        return {"store": s, "model": 2 * lax.rem(x + d + ring, ring) + c}

    barrier = pltpu.get_barrier_semaphore()
    peers = [partner] + [along_y(d) for d in range(1, ring)] + [along_x(d) for d in range(1, ring)]
    for peer in peers:
        pl.semaphore_signal(barrier, inc=1, device_id=peer, device_id_type=MESH_ID)
    pl.semaphore_wait(barrier, len(peers))

    sends = []

    def remote(src, dst, send_sem, recv_sem, peer):
        copy = pltpu.make_async_remote_copy(src_ref=src, dst_ref=dst, send_sem=send_sem, recv_sem=recv_sem,
                                            device_id=peer, device_id_type=MESH_ID)
        copy.start()
        sends.append(copy)
        return copy

    first_stat = remote(stat_ref, st_recv.at[0], st_send.at[0], st_rsem.at[0], partner)

    def direction(st):
        return 1 if st % 2 == 0 else -1

    def block_of(st, k):
        here = s if st < 2 else x
        return lax.rem(here - direction(st) * (k + 1) + 2 * ring, ring)

    def sub_of(st, i):
        here = x if st < 2 else s
        return lax.rem(here - direction(st) * (i + 1) + 2 * ring, ring)

    own_copies, par_copies = {}, {}
    for k in range(ring):
        for st in range(4):
            start, size = quarters[st]
            blk = block_of(st, k)
            slot = st * ring + k

            def view(core):
                if st < 2:
                    return h_ref.at[:, core, blk, pl.ds(start, size), :]
                return h_ref.at[blk, core, :, pl.ds(start, size), :]

            par_copies[st, k] = remote(view(1 - c), par.at[slot, :, pl.ds(0, size), :], p_send.at[slot], p_recv.at[slot], partner)
            mine = pltpu.make_async_copy(view(c), own.at[slot, :, pl.ds(0, size), :], own_sem.at[slot])
            mine.start()
            own_copies[st, k] = mine

    row_id = lax.broadcasted_iota(jnp.int32, (8, LANES), 0)

    def merge(a, b, keep_lm):
        high = jnp.maximum(a[0], b[0])
        total = a[1] * jnp.exp(a[0] - high) + b[1] * jnp.exp(b[0] - high)
        if keep_lm:
            high = jnp.where(row_id == 2, a[0], high)
            total = jnp.where(row_id == 2, a[1], total)
        return high, total

    def load(ref):
        return ref[0:8, :], ref[8:16, :]

    mine = load(stat_ref)
    first_stat.wait_recv()
    theirs = load(st_recv.at[0])
    now = merge(mine, theirs, False)
    for phase, (along, keep_lm) in enumerate(((along_y, True), (along_x, False))):
        st_buf[phase, 0:8, :] = now[0]
        st_buf[phase, 8:16, :] = now[1]
        copies = []
        for d in range(1, ring):
            n = 1 + phase * (ring - 1) + d - 1
            copies.append(remote(st_buf.at[phase], st_recv.at[n], st_send.at[n], st_rsem.at[n], along(d)))
        for d in range(1, ring):
            n = 1 + phase * (ring - 1) + d - 1
            copies[d - 1].wait_recv()
            now = merge(now, load(st_recv.at[n]), keep_lm)
    sout_ref[0:8, :] = now[0]
    sout_ref[8:16, :] = now[1]

    low = lax.broadcasted_iota(jnp.int32, (8, LANES), 1) < LANES // 2
    for who, stat in enumerate((mine, theirs)):
        factor = jnp.exp(stat[0] - now[0])
        for half in range(2):
            row = jnp.broadcast_to(factor[half : half + 1, :], (8, LANES))
            turned = pltpu.roll(row, 64, axis=1)
            fs[who, 2 * half] = jnp.where(low, row, turned)
            fs[who, 2 * half + 1] = jnp.where(low, turned, row)

    ring1_copies, ring2_copies = {}, {}

    def process(st, k, i):
        start, size = quarters[st]
        slot = st * ring + k
        sub = sub_of(st, i)
        band = block_of(st, k) if st < 2 else sub
        if i == 0:
            own_copies[st, k].wait()
            par_copies[st, k].wait_recv()
        if k > 0:
            ring1_copies[st, k - 1, i].wait_recv()
        last = k == ring - 1
        if last and i > 0:
            ring2_copies[st, i - 1].wait_recv()
        f_own = jnp.concatenate([fs[0, band]] * 2, axis=0)
        f_par = jnp.concatenate([fs[1, band]] * 2, axis=0)

        def add(at, count):
            for u in range(count):
                here = pl.ds(pl.multiple_of(at + 16 * u, 16), 16)
                value = own[slot, sub, here, :].astype(F32) * f_own + par[slot, sub, here, :].astype(F32) * f_par
                if k > 0:
                    value = value + ring1[st, k - 1, i, here, :].astype(F32)
                if last and i > 0:
                    value = value + ring2[st, i - 1, here, :].astype(F32)
                if last and i == ring - 1:
                    out_ref[pl.ds(pl.multiple_of(start + at + 16 * u, 16), 16), :] = value
                else:
                    own[slot, sub, here, :] = value.astype(BF16)

        units = size // 16
        full = units // 4

        def body(t, _):
            add(t * 64, 4)
            return 0

        if full:
            lax.fori_loop(0, full, body, 0)
        if units % 4:
            add(full * 64, units % 4)
        d = direction(st)
        if not last:
            peer = along_y(d) if st < 2 else along_x(d)
            ring1_copies[st, k, i] = remote(own.at[slot, sub, pl.ds(0, size), :], ring1.at[st, k, i, pl.ds(0, size), :],
                                            r1_send.at[st, k, i], r1_recv.at[st, k, i], peer)
        elif i < ring - 1:
            peer = along_x(d) if st < 2 else along_y(d)
            ring2_copies[st, i] = remote(own.at[slot, sub, pl.ds(0, size), :], ring2.at[st, i, pl.ds(0, size), :],
                                         r2_send.at[st, i], r2_recv.at[st, i], peer)

    for k in range(ring):
        for i in range(ring):
            for st in range(4):
                process(st, k, i)
    for copy in sends:
        copy.wait_send()


def _quarters(pairs):
    units = pairs // 16
    each = -(-units // 4)
    out, at = [], 0
    for n in range(4):
        size = min(each, units - at)
        out.append((at * 16, size * 16))
        at += size
    return tuple(out)


def solution(mesh):
    store_devs = mesh.shape["store"]
    model_devs = mesh.shape["model"]
    group_axes = ("store", "model")
    cores = 2
    n_x = model_devs // cores
    ring = store_devs

    def local_step(queries, w_head, store_keys, store_tok, temperature, mix_weight):
        vocab_loc = w_head.shape[1]
        vocab = vocab_loc * model_devs
        rows, hidden = queries.shape
        rows_loc = rows // store_devs
        keys = store_keys.shape[0]
        pairs = vocab_loc // 2
        block = min(512, keys)
        n_blocks = keys // block
        shards = (n_x, cores, store_devs, pairs, LANES)
        any_space = pl.BlockSpec(memory_space=pl.ANY)

        packed, stats = pl.pallas_call(
            functools.partial(_scores_kernel, n_blocks, shards),
            grid=(n_blocks,),
            out_shape=(jax.ShapeDtypeStruct(shards, BF16), jax.ShapeDtypeStruct((16, LANES), F32)),
            in_specs=[
                pl.BlockSpec(memory_space=pltpu.SMEM),
                pl.BlockSpec(memory_space=pltpu.SMEM),
                pl.BlockSpec((rows, hidden), lambda i: (0, 0)),
                pl.BlockSpec((block, hidden), lambda i: (i, 0)),
            ],
            out_specs=(any_space, pl.BlockSpec((16, LANES), lambda i: (0, 0))),
            scratch_shapes=[
                pltpu.VMEM((2 * vocab, LANES), F32),
                pltpu.VMEM((2 * keys, LANES), F32),
                pltpu.VMEM((8, rows), F32),
                pltpu.VMEM((2, store_devs, pairs, LANES), BF16),
                pltpu.SemaphoreType.DMA((2,)),
            ],
            compiler_params=pltpu.CompilerParams(vmem_limit_bytes=62 * 1024 * 1024),
            name="local_histogram",
        )(store_tok, (1.0 / temperature).reshape(1), queries, store_keys)

        row_start = lax.axis_index("store") * rows_loc
        my_rows = lax.dynamic_slice_in_dim(queries, row_start, rows_loc, axis=0)
        logits = lax.dot_general(w_head, my_rows, (((0,), (1,)), ((), ())), preferred_element_type=F32)
        lm_top = jnp.max(logits, axis=0)
        lm_sum = jnp.sum(jnp.exp(logits - lm_top), axis=0)
        stats = stats.at[2, :rows_loc].set(lm_top).at[10, :rows_loc].set(lm_sum)

        quarters = _quarters(pairs)
        most = quarters[0][1]
        dma = pltpu.SemaphoreType.DMA
        histogram, totals = pl.pallas_call(
            functools.partial(_exchange_kernel, ring, quarters),
            out_shape=(jax.ShapeDtypeStruct((pairs, LANES), F32), jax.ShapeDtypeStruct((16, LANES), F32)),
            in_specs=[pl.BlockSpec(memory_space=pltpu.VMEM), any_space],
            out_specs=(pl.BlockSpec(memory_space=pltpu.VMEM), pl.BlockSpec(memory_space=pltpu.VMEM)),
            scratch_shapes=[
                pltpu.VMEM((4 * ring, ring, most, LANES), BF16),
                pltpu.VMEM((4 * ring, ring, most, LANES), BF16),
                pltpu.VMEM((4, ring - 1, ring, most, LANES), BF16),
                pltpu.VMEM((4, ring - 1, most, LANES), BF16),
                pltpu.VMEM((2, ring, 8, LANES), F32),
                pltpu.VMEM((2 * ring - 1, 16, LANES), F32),
                pltpu.VMEM((2, 16, LANES), F32),
                dma((4 * ring,)), dma((4 * ring,)), dma((4 * ring,)),
                dma((4, ring - 1, ring)), dma((4, ring - 1, ring)),
                dma((4, ring - 1)), dma((4, ring - 1)),
                dma((2 * ring - 1,)), dma((2 * ring - 1,)),
            ],
            compiler_params=pltpu.CompilerParams(collective_id=0, has_side_effects=True, vmem_limit_bytes=48 * 1024 * 1024),
            name="group_exchange",
        )(stats, packed)

        my_total = lax.dynamic_slice_in_dim(totals[8:10].reshape(2 * LANES), row_start, rows_loc)
        lm_max, lm_total = totals[2, :rows_loc], totals[10, :rows_loc]
        summed = jnp.concatenate([histogram[:, : LANES // 2], histogram[:, LANES // 2 :]], axis=0)
        mixed = mix_weight * (summed / my_total) + (1.0 - mix_weight) * (jnp.exp(logits - lm_max) / lm_total)
        return jnp.log(mixed).T

    return jax.shard_map(local_step, mesh=mesh, in_specs=(P("data", None), P(None, "model"), P(group_axes, None), P(group_axes), P(), P()), out_specs=P(("data", "store"), "model"), check_vma=False)
```

```python
import functools

import jax
import jax.numpy as jnp
from jax import lax
from jax.experimental import pallas as pl
from jax.experimental.pallas import tpu as pltpu
from jax.sharding import PartitionSpec as P

F32 = jnp.float32
BF16 = jnp.bfloat16
LANES = 128
BATCH = 32
GROUP = 16
PACK_TILES = 16
MESH_ID = pl.DeviceIdType.MESH


def _scores_kernel(n_blocks, owners, vocab_loc, tok_ref, rtau_ref, tok2_ref, q_ref, k_ref, h_ref, stat_ref, hist, vals, top, stage, flag_v, flag_s, sem, flag_sem):
    step = pl.program_id(0)
    n_core = h_ref.shape[1]
    first_half = h_ref.shape[3]
    block = k_ref.shape[0]
    rows = q_ref.shape[0]
    keys = vals.shape[0] // 2
    filled = 2 * vocab_loc * owners
    batch, n_batches = tok2_ref.shape

    zero_rows = filled // n_blocks
    hist[pl.ds(pl.multiple_of(step * zero_rows, 8), zero_rows), :] = jnp.zeros((zero_rows, LANES), F32)

    @pl.when(step == 0)
    def _():
        top[...] = jnp.full(top.shape, -jnp.inf, F32)
        rest = hist.shape[0] - filled
        hist[filled:, :] = jnp.zeros((rest, LANES), F32)
        toks = tok2_ref[...]
        same = jnp.zeros(toks.shape, jnp.int32)
        for d in range(1, batch // 2 + 1):
            same = jnp.maximum(same, jnp.where(toks == pltpu.roll(toks, d, axis=0), 1, 0))
        flag_v[...] = jnp.max(same, axis=0, keepdims=True)
        copy = pltpu.make_async_copy(flag_v, flag_s, flag_sem)
        copy.start()
        copy.wait()

    sub = min(256, block)
    for part in range(block // sub):
        key = k_ref[part * sub : (part + 1) * sub, :]
        dots = lax.dot_general(key, q_ref[...], (((1,), (1,)), ((), ())), preferred_element_type=F32)
        wide = key.astype(F32)
        norms = jnp.sum(wide * wide, axis=1, keepdims=True)
        score = (2.0 * dots - norms) * rtau_ref[0]
        top[...] = jnp.maximum(top[...], jnp.max(score.reshape(sub // 8, 8, rows), axis=0))
        base = 2 * (step * block + part * sub)
        for half in range(2):
            vals[pl.ds(base + half, sub, stride=2), :] = score[:, half * LANES : (half + 1) * LANES]

    @pl.when(step == n_blocks - 1)
    def _():
        best = jnp.max(top[...], axis=0, keepdims=True)
        pair = jnp.concatenate([best[:, :LANES], best[:, LANES:]], axis=0)
        best8 = jnp.concatenate([pair] * 4, axis=0)

        def weigh(i, total):
            at = pl.multiple_of(i * 128, 128)
            old = vals[pl.ds(at, 128), :].reshape(16, 8, LANES)
            new = jnp.exp(old - best8[None])
            vals[pl.ds(at, 128), :] = new.reshape(128, LANES)
            return total + jnp.sum(new, axis=0)

        sum8 = lax.fori_loop(0, 2 * keys // 128, weigh, jnp.zeros((8, LANES), F32))
        total = sum8[0:2] + sum8[2:4] + sum8[4:6] + sum8[6:8]
        zeros6 = jnp.zeros((6, LANES), F32)
        stat_ref[...] = jnp.concatenate([pair, zeros6, total, zeros6], axis=0)

        def value(u, i):
            return vals[pl.ds(pl.multiple_of(2 * (u * n_batches + i), 2), 2), :]

        def spots(i, members):
            out = []
            for u in members:
                word = tok_ref[u * n_batches + i]
                for at in (word & 0xFFFF, lax.shift_right_logical(word, 16)):
                    out.append(pl.ds(pl.multiple_of(at, 2), 2))
            return out, [v for u in members for v in (u, u + batch // 2)]

        def scatter(i, _):
            def distinct():
                for first in range(0, batch // 2, GROUP // 2):
                    at, who = spots(i, range(first, first + GROUP // 2))
                    news = [hist[p, :] + value(u, i) for p, u in zip(at, who)]
                    for p, new in zip(at, news):
                        hist[p, :] = new

            def repeated():
                for first in range(batch // 2):
                    for p, u in zip(*spots(i, [first])):
                        hist[p, :] = hist[p, :] + value(u, i)

            lax.cond(flag_s[0, i] > 0, repeated, distinct)
            return 0

        lax.fori_loop(0, n_batches, scatter, 0)

        low = lax.broadcasted_iota(jnp.int32, (16, LANES), 1) < LANES // 2
        tiles = PACK_TILES
        copies = []
        for owner in range(owners):
            slot = owner % 2
            if owner >= 2:
                copies[owner - 2].wait()

            def pack(i, _, owner=owner, slot=slot):
                for u in range(tiles):
                    p = pl.multiple_of(i * (16 * tiles) + u * 16, 16)
                    for half in range(2):
                        a = hist[pl.ds(2 * (owner * vocab_loc + p) + half, 16, stride=2), :]
                        b = hist[pl.ds(2 * (owner * vocab_loc + first_half + p) + half, 16, stride=2), :]
                        stage[slot, 2 * half, pl.ds(p, 16), :] = jnp.where(low, a, pltpu.roll(b, 64, axis=1)).astype(BF16)
                        stage[slot, 2 * half + 1, pl.ds(p, 16), :] = jnp.where(low, pltpu.roll(a, 64, axis=1), b).astype(BF16)
                return 0

            lax.fori_loop(0, first_half // (16 * tiles), pack, 0)
            copy = pltpu.make_async_copy(stage.at[slot], h_ref.at[owner // n_core, owner % n_core], sem.at[slot])
            copy.start()
            copies.append(copy)
        copies[-2].wait()
        copies[-1].wait()


def _exchange_kernel(ring, vocab_loc, lam_ref, stat_ref, q_ref, h_ref, w_ref, out_ref,
                     own, par, ring1, ring2, wbuf, logit, fin, qpad, lm_top, fs, st_recv, st_buf, lm_recv, lm_buf,
                     own_sem, p_send, p_recv, r1_send, r1_recv, r2_send, r2_recv, st_send, st_rsem, lm_send, lm_rsem, w_sem):
    s = lax.axis_index("store")
    m = lax.axis_index("model")
    x = lax.div(m, 2)
    c = lax.rem(m, 2)
    size = own.shape[2]
    first_half = 4 * size
    second_half = vocab_loc - first_half
    partner = {"store": s, "model": 2 * x + 1 - c}

    def along_y(d):
        return {"store": lax.rem(s + d + ring, ring), "model": m}

    def along_x(d):
        return {"store": s, "model": 2 * lax.rem(x + d + ring, ring) + c}

    barrier = pltpu.get_barrier_semaphore()
    peers = [partner] + [along_y(d) for d in range(1, ring)] + [along_x(d) for d in range(1, ring)]
    for peer in peers:
        pl.semaphore_signal(barrier, inc=1, device_id=peer, device_id_type=MESH_ID)
    pl.semaphore_wait(barrier, len(peers))

    sends = []

    def remote(src, dst, send_sem, recv_sem, peer):
        copy = pltpu.make_async_remote_copy(src_ref=src, dst_ref=dst, send_sem=send_sem, recv_sem=recv_sem,
                                            device_id=peer, device_id_type=MESH_ID)
        copy.start()
        sends.append(copy)
        return copy

    first_stat = remote(stat_ref, st_recv.at[0], st_send.at[0], st_rsem.at[0], partner)

    def direction(st):
        return 1 if st % 2 == 0 else -1

    def block_of(st, k):
        here = s if st < 2 else x
        return lax.rem(here - direction(st) * (k + 1) + 2 * ring, ring)

    def sub_of(st, i):
        here = x if st < 2 else s
        return lax.rem(here - direction(st) * (i + 1) + 2 * ring, ring)

    w_copies = {}

    def start_w(q):
        for half in range(2):
            count = size if half == 0 else min(size, second_half - q * size)
            if count <= 0:
                continue
            at = half * first_half + q * size
            copy = pltpu.make_async_copy(w_ref.at[pl.ds(at, count), :], wbuf.at[pl.ds(at, count), :], w_sem.at[half, q])
            copy.start()
            w_copies[q, half] = copy

    own_copies, par_copies = {}, {}
    for k in range(ring):
        for st in range(4):
            blk = block_of(st, k)
            slot = st * ring + k

            def view(core):
                if st < 2:
                    return h_ref.at[:, core, blk, pl.ds(st * size, size), :]
                return h_ref.at[blk, core, :, pl.ds(st * size, size), :]

            par_copies[st, k] = remote(view(1 - c), par.at[slot], p_send.at[slot], p_recv.at[slot], partner)
            mine = pltpu.make_async_copy(view(c), own.at[slot], own_sem.at[slot])
            mine.start()
            own_copies[st, k] = mine
        start_w(k)

    if second_half < first_half:
        wbuf[vocab_loc:, :] = jnp.zeros((2 * first_half - vocab_loc, wbuf.shape[1]), BF16)
    my_rows = q_ref[pl.ds(pl.multiple_of(s * 64, 64), 64), :]
    blank = jnp.zeros(my_rows.shape, BF16)
    qpad[0, 0:64, :] = my_rows
    qpad[0, 64:128, :] = blank
    qpad[1, 0:64, :] = blank
    qpad[1, 64:128, :] = my_rows

    def merge(a, b):
        high = jnp.maximum(a[0], b[0])
        return high, a[1] * jnp.exp(a[0] - high) + b[1] * jnp.exp(b[0] - high)

    def load(ref):
        return ref[0:8, :], ref[8:16, :]

    mine = load(stat_ref)
    first_stat.wait_recv()
    theirs = load(st_recv.at[0])
    now = merge(mine, theirs)
    for phase, along in enumerate((along_y, along_x)):
        st_buf[phase, 0:8, :] = now[0]
        st_buf[phase, 8:16, :] = now[1]
        copies = []
        for d in range(1, ring):
            n = 1 + phase * (ring - 1) + d - 1
            copies.append(remote(st_buf.at[phase], st_recv.at[n], st_send.at[n], st_rsem.at[n], along(d)))
        for d in range(1, ring):
            n = 1 + phase * (ring - 1) + d - 1
            copies[d - 1].wait_recv()
            now = merge(now, load(st_recv.at[n]))

    low = lax.broadcasted_iota(jnp.int32, (8, LANES), 1) < LANES // 2

    def spread(who, table):
        for half in range(2):
            row = jnp.broadcast_to(table[half : half + 1, :], (8, LANES))
            turned = pltpu.roll(row, 64, axis=1)
            fs[who, 2 * half] = jnp.where(low, row, turned)
            fs[who, 2 * half + 1] = jnp.where(low, turned, row)

    spread(0, jnp.exp(mine[0] - now[0]))
    spread(1, jnp.exp(theirs[0] - now[0]))
    spread(2, now[1])
    lam = lam_ref[0]

    ring1_copies, ring2_copies = {}, {}

    def process(st, k, i):
        slot = st * ring + k
        sub = sub_of(st, i)
        band = block_of(st, k) if st < 2 else sub
        if i == 0:
            own_copies[st, k].wait()
            par_copies[st, k].wait_recv()
        if k > 0:
            ring1_copies[st, k - 1, i].wait_recv()
        last = k == ring - 1
        if last and i > 0:
            ring2_copies[st, i - 1].wait_recv()
        f_own = jnp.concatenate([fs[0, band]] * 2, axis=0)
        f_par = jnp.concatenate([fs[1, band]] * 2, axis=0)
        unroll = 8 if size % 128 == 0 else 1

        def body(t, _):
            for u in range(unroll):
                here = pl.ds(pl.multiple_of(t * (16 * unroll) + 16 * u, 16), 16)
                value = own[slot, sub, here, :].astype(F32) * f_own + par[slot, sub, here, :].astype(F32) * f_par
                if k > 0:
                    value = value + ring1[st, k - 1, i, here, :].astype(F32)
                if last and i > 0:
                    value = value + ring2[st, i - 1, here, :].astype(F32)
                if last and i == ring - 1:
                    fin[here, :] = value
                else:
                    own[slot, sub, here, :] = value.astype(BF16)
            return 0

        lax.fori_loop(0, size // (16 * unroll), body, 0)
        d = direction(st)
        if not last:
            peer = along_y(d) if st < 2 else along_x(d)
            ring1_copies[st, k, i] = remote(own.at[slot, sub], ring1.at[st, k, i], r1_send.at[st, k, i], r1_recv.at[st, k, i], peer)
        elif i < ring - 1:
            peer = along_x(d) if st < 2 else along_y(d)
            ring2_copies[st, i] = remote(own.at[slot, sub], ring2.at[st, i], r2_send.at[st, i], r2_recv.at[st, i], peer)
        else:
            finish(st)

    def head(q):
        for half in range(2):
            if (q, half) in w_copies:
                w_copies[q, half].wait()
        contract = (((1,), (1,)), ((), ()))
        at = q * size
        part = lax.dot_general(wbuf[at : at + size, :], qpad[0], contract, preferred_element_type=F32)
        part = part + lax.dot_general(wbuf[first_half + at : first_half + at + size, :], qpad[1], contract, preferred_element_type=F32)
        if at + size > second_half:
            row = lax.broadcasted_iota(jnp.int32, (size, LANES), 0) + at
            lane = lax.broadcasted_iota(jnp.int32, (size, LANES), 1)
            part = jnp.where((row >= second_half) & (lane >= LANES // 2), -jnp.inf, part)
        logit[at : at + size, :] = part
        best = jnp.max(part.reshape(size // 8, 8, LANES), axis=0)
        lm_top[...] = best if q == 0 else jnp.maximum(lm_top[...], best)

    lm = {}

    def lm_local():
        best = jnp.max(lm_top[...], axis=0, keepdims=True)
        best = jnp.broadcast_to(best, (8, LANES))
        best = jnp.maximum(best, pltpu.roll(best, 64, axis=1))

        def body(t, total):
            here = pl.ds(pl.multiple_of(t * 64, 64), 64)
            new = jnp.exp(logit[here, :].reshape(8, 8, LANES) - best[None])
            logit[here, :] = new.reshape(64, LANES)
            return total + jnp.sum(new, axis=0)

        total = lax.fori_loop(0, first_half // 64, body, jnp.zeros((8, LANES), F32))
        total = jnp.broadcast_to(jnp.sum(total, axis=0, keepdims=True), (8, LANES))
        total = total + pltpu.roll(total, 64, axis=1)
        lm["mine"] = lm["now"] = (best, total)
        lm_publish(0, [partner])

    def lm_publish(phase, targets):
        lm_buf[phase, 0:8, :] = lm["now"][0]
        lm_buf[phase, 8:16, :] = lm["now"][1]
        lm["copies"] = [remote(lm_buf.at[phase], lm_recv.at[phase + n], lm_send.at[phase + n], lm_rsem.at[phase + n], peer)
                        for n, peer in enumerate(targets)]
        lm["slots"] = [phase + n for n in range(len(targets))]

    def lm_collect():
        for copy, n in zip(lm["copies"], lm["slots"]):
            copy.wait_recv()
            lm["now"] = merge(lm["now"], load(lm_recv.at[n]))

    def finish(st):
        scale = lam / fs[2, s]
        lm_scale = lm["scale"]
        wide = min(LANES, size)
        for b in range(size // wide):
            at = st * size + b * wide
            p_knn = fin[b * wide : (b + 1) * wide, :].reshape(wide // 8, 8, LANES) * scale[None]
            p_lm = logit[at : at + wide, :].reshape(wide // 8, 8, LANES) * lm_scale[None]
            mixed = jnp.log(p_knn + p_lm).reshape(wide, LANES).T
            out_ref[:, at : at + wide] = mixed[0:64, :]
            count = min(wide, second_half - at)
            if count > 0:
                out_ref[:, first_half + at : first_half + at + count] = mixed[64:128, :count]

    for k in range(ring):
        for i in range(ring):
            for st in range(4):
                process(st, k, i)
            if k == 0:
                head(i)
            if k == 1 and i == 0:
                lm_local()
            if k == 2 and i == 0:
                lm_collect()
                lm_publish(1, [along_x(d) for d in range(1, ring)])
            if k == 3 and i == 0:
                lm_collect()
                lm["scale"] = (1.0 - lam) * jnp.exp(lm["mine"][0] - lm["now"][0]) / lm["now"][1]
    for copy in sends:
        copy.wait_send()


def solution(mesh):
    store_devs = mesh.shape["store"]
    model_devs = mesh.shape["model"]
    group_axes = ("store", "model")
    cores = 2
    n_x = model_devs // cores
    ring = store_devs

    def local_step(queries, w_head, store_keys, store_tok, temperature, mix_weight):
        vocab_loc = w_head.shape[1]
        rows, hidden = queries.shape
        rows_loc = rows // store_devs
        keys = store_keys.shape[0]
        first_half = -(-vocab_loc // (2 * 4 * LANES)) * 4 * LANES
        size = first_half // 4
        block = min(512, keys)
        n_blocks = keys // block
        n_batches = keys // BATCH
        hist_rows = 2 * ((model_devs - 1) * vocab_loc + 2 * first_half)
        assert 2 * vocab_loc * model_devs <= 1 << 16
        words = 2 * store_tok[: keys // 2] | (2 * store_tok[keys // 2 :] << 16)
        any_space = pl.BlockSpec(memory_space=pl.ANY)
        smem = pl.BlockSpec(memory_space=pltpu.SMEM)
        vmem = pl.BlockSpec(memory_space=pltpu.VMEM)
        dma = pltpu.SemaphoreType.DMA

        packed, stats = pl.pallas_call(
            functools.partial(_scores_kernel, n_blocks, model_devs, vocab_loc),
            grid=(n_blocks,),
            out_shape=(jax.ShapeDtypeStruct((n_x, cores, store_devs, first_half, LANES), BF16), jax.ShapeDtypeStruct((16, LANES), F32)),
            in_specs=[
                smem,
                smem,
                pl.BlockSpec((BATCH, n_batches), lambda i: (0, 0)),
                pl.BlockSpec((rows, hidden), lambda i: (0, 0)),
                pl.BlockSpec((block, hidden), lambda i: (i, 0)),
            ],
            out_specs=(any_space, pl.BlockSpec((16, LANES), lambda i: (0, 0))),
            scratch_shapes=[
                pltpu.VMEM((hist_rows, LANES), F32),
                pltpu.VMEM((2 * keys, LANES), F32),
                pltpu.VMEM((8, rows), F32),
                pltpu.VMEM((2, store_devs, first_half, LANES), BF16),
                pltpu.VMEM((1, n_batches), jnp.int32),
                pltpu.SMEM((1, n_batches), jnp.int32),
                dma((2,)),
                dma,
            ],
            compiler_params=pltpu.CompilerParams(vmem_limit_bytes=62 * 1024 * 1024),
            name="local_histogram",
        )(words, (1.0 / temperature).reshape(1), store_tok.reshape(BATCH, n_batches), queries, store_keys)

        return pl.pallas_call(
            functools.partial(_exchange_kernel, ring, vocab_loc),
            out_shape=jax.ShapeDtypeStruct((rows_loc, vocab_loc), F32),
            in_specs=[smem, vmem, vmem, any_space, any_space],
            out_specs=vmem,
            scratch_shapes=[
                pltpu.VMEM((4 * ring, ring, size, LANES), BF16),
                pltpu.VMEM((4 * ring, ring, size, LANES), BF16),
                pltpu.VMEM((4, ring - 1, ring, size, LANES), BF16),
                pltpu.VMEM((4, ring - 1, size, LANES), BF16),
                pltpu.VMEM((2 * first_half, hidden), BF16),
                pltpu.VMEM((first_half, LANES), F32),
                pltpu.VMEM((size, LANES), F32),
                pltpu.VMEM((2, LANES, hidden), BF16),
                pltpu.VMEM((8, LANES), F32),
                pltpu.VMEM((3, ring, 8, LANES), F32),
                pltpu.VMEM((2 * ring - 1, 16, LANES), F32),
                pltpu.VMEM((2, 16, LANES), F32),
                pltpu.VMEM((ring, 16, LANES), F32),
                pltpu.VMEM((2, 16, LANES), F32),
                dma((4 * ring,)), dma((4 * ring,)), dma((4 * ring,)),
                dma((4, ring - 1, ring)), dma((4, ring - 1, ring)),
                dma((4, ring - 1)), dma((4, ring - 1)),
                dma((2 * ring - 1,)), dma((2 * ring - 1,)),
                dma((ring,)), dma((ring,)),
                dma((2, 4)),
            ],
            compiler_params=pltpu.CompilerParams(collective_id=0, has_side_effects=True, vmem_limit_bytes=62 * 1024 * 1024),
            name="group_exchange",
        )(mix_weight.reshape(1), stats, queries, packed, w_head.T)

    return jax.shard_map(local_step, mesh=mesh, in_specs=(P("data", None), P(None, "model"), P(group_axes, None), P(group_axes), P(), P()), out_specs=P(("data", "store"), "model"), check_vma=False)
```

```python
import functools

import jax
import jax.numpy as jnp
from jax import lax
from jax.experimental import pallas as pl
from jax.experimental.pallas import tpu as pltpu
from jax.sharding import PartitionSpec as P

F32 = jnp.float32
BF16 = jnp.bfloat16
LANES = 128
BATCH = 32
GROUP = 16
PACK_TILES = 16
MESH_ID = pl.DeviceIdType.MESH
ORDER = ((0, 0), (0, 1), (0, 2), (1, 0), (0, 3), (1, 1), (2, 0), (1, 2), (2, 1), (3, 0), (1, 3), (2, 2), (3, 1), (2, 3), (3, 2), (3, 3))


def _scores_kernel(n_blocks, owners, vocab_loc, tok_ref, rtau_ref, tok2_ref, q_ref, k_ref, h_ref, stat_ref, hist, vals, top, stage, flag_v, flag_s, sem, flag_sem):
    step = pl.program_id(0)
    n_core = h_ref.shape[1]
    first_half = h_ref.shape[3]
    block = k_ref.shape[0]
    rows = q_ref.shape[0]
    keys = vals.shape[0] // 2
    filled = 2 * vocab_loc * owners
    batch, n_batches = tok2_ref.shape

    zero_rows = filled // n_blocks
    hist[pl.ds(pl.multiple_of(step * zero_rows, 8), zero_rows), :] = jnp.zeros((zero_rows, LANES), F32)

    @pl.when(step == 0)
    def _():
        top[...] = jnp.full(top.shape, -jnp.inf, F32)
        rest = hist.shape[0] - filled
        hist[filled:, :] = jnp.zeros((rest, LANES), F32)
        toks = tok2_ref[...]
        same = jnp.zeros(toks.shape, jnp.int32)
        for d in range(1, batch // 2 + 1):
            same = jnp.maximum(same, jnp.where(toks == pltpu.roll(toks, d, axis=0), 1, 0))
        flag_v[...] = jnp.max(same, axis=0, keepdims=True)
        copy = pltpu.make_async_copy(flag_v, flag_s, flag_sem)
        copy.start()
        copy.wait()

    sub = min(256, block)
    for part in range(block // sub):
        key = k_ref[part * sub : (part + 1) * sub, :]
        dots = lax.dot_general(key, q_ref[...], (((1,), (1,)), ((), ())), preferred_element_type=F32)
        wide = key.astype(F32)
        norms = jnp.sum(wide * wide, axis=1, keepdims=True)
        score = (2.0 * dots - norms) * rtau_ref[0]
        top[...] = jnp.maximum(top[...], jnp.max(score.reshape(sub // 8, 8, rows), axis=0))
        base = 2 * (step * block + part * sub)
        for half in range(2):
            vals[pl.ds(base + half, sub, stride=2), :] = score[:, half * LANES : (half + 1) * LANES]

    @pl.when(step == n_blocks - 1)
    def _():
        best = jnp.max(top[...], axis=0, keepdims=True)
        pair = jnp.concatenate([best[:, :LANES], best[:, LANES:]], axis=0)
        best8 = jnp.concatenate([pair] * 4, axis=0)

        def weigh(i, total):
            at = pl.multiple_of(i * 128, 128)
            old = vals[pl.ds(at, 128), :].reshape(16, 8, LANES)
            new = jnp.exp(old - best8[None])
            vals[pl.ds(at, 128), :] = new.reshape(128, LANES)
            return total + jnp.sum(new, axis=0)

        sum8 = lax.fori_loop(0, 2 * keys // 128, weigh, jnp.zeros((8, LANES), F32))
        total = sum8[0:2] + sum8[2:4] + sum8[4:6] + sum8[6:8]
        zeros6 = jnp.zeros((6, LANES), F32)
        stat_ref[...] = jnp.concatenate([pair, zeros6, total, zeros6], axis=0)

        def value(u, i):
            return vals[pl.ds(pl.multiple_of(2 * (u * n_batches + i), 2), 2), :]

        def spots(i, members):
            out = []
            for u in members:
                word = tok_ref[u * n_batches + i]
                for at in (word & 0xFFFF, lax.shift_right_logical(word, 16)):
                    out.append(pl.ds(pl.multiple_of(at, 2), 2))
            return out, [v for u in members for v in (u, u + batch // 2)]

        def scatter(i, _):
            def distinct():
                for first in range(0, batch // 2, GROUP // 2):
                    at, who = spots(i, range(first, first + GROUP // 2))
                    news = [hist[p, :] + value(u, i) for p, u in zip(at, who)]
                    for p, new in zip(at, news):
                        hist[p, :] = new

            def repeated():
                for first in range(batch // 2):
                    for p, u in zip(*spots(i, [first])):
                        hist[p, :] = hist[p, :] + value(u, i)

            lax.cond(flag_s[0, i] > 0, repeated, distinct)
            return 0

        lax.fori_loop(0, n_batches, scatter, 0)

        low = lax.broadcasted_iota(jnp.int32, (16, LANES), 1) < LANES // 2
        tiles = PACK_TILES
        copies = []
        for owner in range(owners):
            slot = owner % 2
            if owner >= 2:
                copies[owner - 2].wait()

            def pack(i, _, owner=owner, slot=slot):
                for u in range(tiles):
                    p = pl.multiple_of(i * (16 * tiles) + u * 16, 16)
                    for half in range(2):
                        a = hist[pl.ds(2 * (owner * vocab_loc + p) + half, 16, stride=2), :]
                        b = hist[pl.ds(2 * (owner * vocab_loc + first_half + p) + half, 16, stride=2), :]
                        stage[slot, 2 * half, pl.ds(p, 16), :] = jnp.where(low, a, pltpu.roll(b, 64, axis=1)).astype(BF16)
                        stage[slot, 2 * half + 1, pl.ds(p, 16), :] = jnp.where(low, pltpu.roll(a, 64, axis=1), b).astype(BF16)
                return 0

            lax.fori_loop(0, first_half // (16 * tiles), pack, 0)
            copy = pltpu.make_async_copy(stage.at[slot], h_ref.at[owner // n_core, owner % n_core], sem.at[slot])
            copy.start()
            copies.append(copy)
        copies[-2].wait()
        copies[-1].wait()


def _exchange_kernel(ring, vocab_loc, lam_ref, stat_ref, q_ref, h_ref, w_ref, out_ref,
                     own, par, ring1, ring2, wbuf, logit, fin, qpad, lm_top, fs, st_recv, st_buf, lm_recv, lm_buf,
                     own_sem, p_send, p_recv, r1_send, r1_recv, r2_send, r2_recv, st_send, st_rsem, lm_send, lm_rsem, w_sem):
    s = lax.axis_index("store")
    m = lax.axis_index("model")
    x = lax.div(m, 2)
    c = lax.rem(m, 2)
    size = own.shape[2]
    first_half = 4 * size
    second_half = vocab_loc - first_half
    partner = {"store": s, "model": 2 * x + 1 - c}

    def along_y(d):
        return {"store": lax.rem(s + d + ring, ring), "model": m}

    def along_x(d):
        return {"store": s, "model": 2 * lax.rem(x + d + ring, ring) + c}

    barrier = pltpu.get_barrier_semaphore()
    peers = [partner] + [along_y(d) for d in range(1, ring)] + [along_x(d) for d in range(1, ring)]
    for peer in peers:
        pl.semaphore_signal(barrier, inc=1, device_id=peer, device_id_type=MESH_ID)
    pl.semaphore_wait(barrier, len(peers))

    sends = []

    def remote(src, dst, send_sem, recv_sem, peer):
        copy = pltpu.make_async_remote_copy(src_ref=src, dst_ref=dst, send_sem=send_sem, recv_sem=recv_sem,
                                            device_id=peer, device_id_type=MESH_ID)
        copy.start()
        sends.append(copy)
        return copy

    first_stat = remote(stat_ref, st_recv.at[0], st_send.at[0], st_rsem.at[0], partner)

    def direction(st):
        return 1 if st % 2 == 0 else -1

    def block_of(st, k):
        here = s if st < 2 else x
        return lax.rem(here - direction(st) * (k + 1) + 2 * ring, ring)

    def sub_of(st, i):
        here = x if st < 2 else s
        return lax.rem(here - direction(st) * (i + 1) + 2 * ring, ring)

    w_copies = {}

    def start_w(q):
        for half in range(2):
            count = size if half == 0 else min(size, second_half - q * size)
            if count <= 0:
                continue
            at = half * first_half + q * size
            copy = pltpu.make_async_copy(w_ref.at[pl.ds(at, count), :], wbuf.at[pl.ds(at, count), :], w_sem.at[half, q])
            copy.start()
            w_copies[q, half] = copy

    own_copies, par_copies = {}, {}

    def fetch(st, k, sub, sem):
        blk = block_of(st, k)
        slot = st * ring + k
        rows = pl.ds(st * size, size)

        def view(core):
            if sub is None:
                return h_ref.at[:, core, blk, rows, :] if st < 2 else h_ref.at[blk, core, :, rows, :]
            return h_ref.at[sub, core, blk, rows, :] if st < 2 else h_ref.at[blk, core, sub, rows, :]

        def into(ref):
            return ref.at[slot] if sub is None else ref.at[slot, sub]

        par_copies[st, sem] = remote(view(1 - c), into(par), p_send.at[st, sem], p_recv.at[st, sem], partner)
        mine = pltpu.make_async_copy(view(c), into(own), own_sem.at[st, sem])
        mine.start()
        own_copies[st, sem] = mine

    for i in range(ring):
        for st in range(4):
            fetch(st, 0, sub_of(st, i), i)
    for k in range(1, ring):
        start_w(k - 1)
        for st in range(4):
            fetch(st, k, None, ring + k - 1)
    start_w(ring - 1)

    if second_half < first_half:
        wbuf[vocab_loc:, :] = jnp.zeros((2 * first_half - vocab_loc, wbuf.shape[1]), BF16)
    my_rows = q_ref[pl.ds(pl.multiple_of(s * 64, 64), 64), :]
    blank = jnp.zeros(my_rows.shape, BF16)
    qpad[0, 0:64, :] = my_rows
    qpad[0, 64:128, :] = blank
    qpad[1, 0:64, :] = blank
    qpad[1, 64:128, :] = my_rows

    def merge(a, b):
        high = jnp.maximum(a[0], b[0])
        return high, a[1] * jnp.exp(a[0] - high) + b[1] * jnp.exp(b[0] - high)

    def load(ref):
        return ref[0:8, :], ref[8:16, :]

    low = lax.broadcasted_iota(jnp.int32, (8, LANES), 1) < LANES // 2

    def spread(who, table):
        for half in range(2):
            row = jnp.broadcast_to(table[half : half + 1, :], (8, LANES))
            turned = pltpu.roll(row, 64, axis=1)
            fs[who, 2 * half] = jnp.where(low, row, turned)
            fs[who, 2 * half + 1] = jnp.where(low, turned, row)

    mine = load(stat_ref)
    first_stat.wait_recv()
    theirs = load(st_recv.at[0])
    knn = {"now": merge(mine, theirs)}
    spread(0, jnp.exp(mine[0] - knn["now"][0]))
    spread(1, jnp.exp(theirs[0] - knn["now"][0]))

    def knn_publish(phase, targets):
        st_buf[phase, 0:8, :] = knn["now"][0]
        st_buf[phase, 8:16, :] = knn["now"][1]
        knn["copies"] = []
        for n, peer in targets:
            knn["copies"].append((n, remote(st_buf.at[phase], st_recv.at[n], st_send.at[n], st_rsem.at[n], peer)))

    def knn_collect():
        for n, copy in knn["copies"]:
            copy.wait_recv()
            if n < 2 * ring - 1:
                knn["now"] = merge(knn["now"], load(st_recv.at[n]))

    side = 2 * ring - 1
    knn_publish(0, [(d, along_y(d)) for d in range(1, ring)] + [(side, along_x(1)), (side + 1, along_x(-1))])

    def knn_group():
        knn_collect()
        high = knn["now"][0]
        spread(2, jnp.exp(mine[0] - high))
        spread(3, jnp.exp(theirs[0] - high))
        spread(4, knn["now"][1])
        for st, n in enumerate((1, ring - 1, side, side + 1)):
            spread(5 + st, jnp.exp(st_recv[n, 0:8, :] - high))

    lam = lam_ref[0]

    ring1_copies, ring2_copies = {}, {}

    def process(st, k, i):
        slot = st * ring + k
        sub = sub_of(st, i)
        band = block_of(st, k) if st < 2 else sub
        if k == 0 or i == 0:
            sem = i if k == 0 else ring + k - 1
            own_copies[st, sem].wait()
            par_copies[st, sem].wait_recv()
        if k > 0:
            ring1_copies[st, k - 1, i].wait_recv()
        last = k == ring - 1
        if last and i > 0:
            ring2_copies[st, i - 1].wait_recv()
        f_own = jnp.concatenate([fs[0 if k == 0 else 2, band]] * 2, axis=0)
        f_par = jnp.concatenate([fs[1 if k == 0 else 3, band]] * 2, axis=0)
        f_ring = jnp.concatenate([fs[5 + st, band]] * 2, axis=0) if k == 1 else None
        unroll = 8 if size % 128 == 0 else 1

        def body(t, _):
            for u in range(unroll):
                here = pl.ds(pl.multiple_of(t * (16 * unroll) + 16 * u, 16), 16)
                value = own[slot, sub, here, :].astype(F32) * f_own + par[slot, sub, here, :].astype(F32) * f_par
                if k > 0:
                    came = ring1[st, k - 1, i, here, :].astype(F32)
                    value = value + (came * f_ring if k == 1 else came)
                if last and i > 0:
                    value = value + ring2[st, i - 1, here, :].astype(F32)
                if last and i == ring - 1:
                    fin[here, :] = value
                else:
                    own[slot, sub, here, :] = value.astype(BF16)
            return 0

        lax.fori_loop(0, size // (16 * unroll), body, 0)
        d = direction(st)
        if not last:
            peer = along_y(d) if st < 2 else along_x(d)
            ring1_copies[st, k, i] = remote(own.at[slot, sub], ring1.at[st, k, i], r1_send.at[st, k, i], r1_recv.at[st, k, i], peer)
        elif i < ring - 1:
            peer = along_x(d) if st < 2 else along_y(d)
            ring2_copies[st, i] = remote(own.at[slot, sub], ring2.at[st, i], r2_send.at[st, i], r2_recv.at[st, i], peer)
        else:
            finish(st)

    def head(q):
        for half in range(2):
            if (q, half) in w_copies:
                w_copies[q, half].wait()
        contract = (((1,), (1,)), ((), ()))
        at = q * size
        part = lax.dot_general(wbuf[at : at + size, :], qpad[0], contract, preferred_element_type=F32)
        part = part + lax.dot_general(wbuf[first_half + at : first_half + at + size, :], qpad[1], contract, preferred_element_type=F32)
        if at + size > second_half:
            row = lax.broadcasted_iota(jnp.int32, (size, LANES), 0) + at
            lane = lax.broadcasted_iota(jnp.int32, (size, LANES), 1)
            part = jnp.where((row >= second_half) & (lane >= LANES // 2), -jnp.inf, part)
        logit[at : at + size, :] = part
        best = jnp.max(part.reshape(size // 8, 8, LANES), axis=0)
        lm_top[...] = best if q == 0 else jnp.maximum(lm_top[...], best)

    lm = {}

    def lm_local():
        best = jnp.max(lm_top[...], axis=0, keepdims=True)
        best = jnp.broadcast_to(best, (8, LANES))
        best = jnp.maximum(best, pltpu.roll(best, 64, axis=1))

        def body(t, total):
            here = pl.ds(pl.multiple_of(t * 64, 64), 64)
            new = jnp.exp(logit[here, :].reshape(8, 8, LANES) - best[None])
            logit[here, :] = new.reshape(64, LANES)
            return total + jnp.sum(new, axis=0)

        total = lax.fori_loop(0, first_half // 64, body, jnp.zeros((8, LANES), F32))
        total = jnp.broadcast_to(jnp.sum(total, axis=0, keepdims=True), (8, LANES))
        total = total + pltpu.roll(total, 64, axis=1)
        lm["mine"] = lm["now"] = (best, total)
        lm_publish(0, [partner])

    def lm_publish(phase, targets):
        lm_buf[phase, 0:8, :] = lm["now"][0]
        lm_buf[phase, 8:16, :] = lm["now"][1]
        lm["copies"] = [remote(lm_buf.at[phase], lm_recv.at[phase + n], lm_send.at[phase + n], lm_rsem.at[phase + n], peer)
                        for n, peer in enumerate(targets)]
        lm["slots"] = [phase + n for n in range(len(targets))]

    def lm_collect():
        for copy, n in zip(lm["copies"], lm["slots"]):
            copy.wait_recv()
            lm["now"] = merge(lm["now"], load(lm_recv.at[n]))

    def finish(st):
        scale = lam / fs[4, s]
        lm_scale = lm["scale"]
        wide = min(LANES, size)
        for b in range(size // wide):
            at = st * size + b * wide
            p_knn = fin[b * wide : (b + 1) * wide, :].reshape(wide // 8, 8, LANES) * scale[None]
            p_lm = logit[at : at + wide, :].reshape(wide // 8, 8, LANES) * lm_scale[None]
            mixed = jnp.log(p_knn + p_lm).reshape(wide, LANES).T
            out_ref[:, at : at + wide] = mixed[0:64, :]
            count = min(wide, second_half - at)
            if count > 0:
                out_ref[:, first_half + at : first_half + at + count] = mixed[64:128, :count]

    for place, (k, i) in enumerate(ORDER):
        for st in range(4):
            process(st, k, i)
        if place == 0:
            knn_collect()
            knn_publish(1, [(ring - 1 + d, along_x(d)) for d in range(1, ring)])
        if place == 2:
            knn_group()
        if place in (3, 4, 6, 7):
            head((3, 4, 6, 7).index(place))
        if place == 8:
            lm_local()
        if place == 10:
            lm_collect()
            lm_publish(1, [along_x(d) for d in range(1, ring)])
        if place == 12:
            lm_collect()
            lm["scale"] = (1.0 - lam) * jnp.exp(lm["mine"][0] - lm["now"][0]) / lm["now"][1]
    for copy in sends:
        copy.wait_send()


def solution(mesh):
    store_devs = mesh.shape["store"]
    model_devs = mesh.shape["model"]
    group_axes = ("store", "model")
    cores = 2
    n_x = model_devs // cores
    ring = store_devs

    def local_step(queries, w_head, store_keys, store_tok, temperature, mix_weight):
        vocab_loc = w_head.shape[1]
        rows, hidden = queries.shape
        rows_loc = rows // store_devs
        keys = store_keys.shape[0]
        first_half = -(-vocab_loc // (2 * 4 * LANES)) * 4 * LANES
        size = first_half // 4
        block = min(1024, keys)
        n_blocks = keys // block
        n_batches = keys // BATCH
        hist_rows = 2 * ((model_devs - 1) * vocab_loc + 2 * first_half)
        assert 2 * vocab_loc * model_devs <= 1 << 16
        words = 2 * store_tok[: keys // 2] | (2 * store_tok[keys // 2 :] << 16)
        any_space = pl.BlockSpec(memory_space=pl.ANY)
        smem = pl.BlockSpec(memory_space=pltpu.SMEM)
        vmem = pl.BlockSpec(memory_space=pltpu.VMEM)
        dma = pltpu.SemaphoreType.DMA

        packed, stats = pl.pallas_call(
            functools.partial(_scores_kernel, n_blocks, model_devs, vocab_loc),
            grid=(n_blocks,),
            out_shape=(jax.ShapeDtypeStruct((n_x, cores, store_devs, first_half, LANES), BF16), jax.ShapeDtypeStruct((16, LANES), F32)),
            in_specs=[
                smem,
                smem,
                pl.BlockSpec((BATCH, n_batches), lambda i: (0, 0)),
                pl.BlockSpec((rows, hidden), lambda i: (0, 0)),
                pl.BlockSpec((block, hidden), lambda i: (i, 0)),
            ],
            out_specs=(any_space, pl.BlockSpec((16, LANES), lambda i: (0, 0))),
            scratch_shapes=[
                pltpu.VMEM((hist_rows, LANES), F32),
                pltpu.VMEM((2 * keys, LANES), F32),
                pltpu.VMEM((8, rows), F32),
                pltpu.VMEM((2, store_devs, first_half, LANES), BF16),
                pltpu.VMEM((1, n_batches), jnp.int32),
                pltpu.SMEM((1, n_batches), jnp.int32),
                dma((2,)),
                dma,
            ],
            compiler_params=pltpu.CompilerParams(vmem_limit_bytes=62 * 1024 * 1024),
            name="local_histogram",
        )(words, (1.0 / temperature).reshape(1), store_tok.reshape(BATCH, n_batches), queries, store_keys)

        return pl.pallas_call(
            functools.partial(_exchange_kernel, ring, vocab_loc),
            out_shape=jax.ShapeDtypeStruct((rows_loc, vocab_loc), F32),
            in_specs=[smem, vmem, vmem, any_space, any_space],
            out_specs=vmem,
            scratch_shapes=[
                pltpu.VMEM((4 * ring, ring, size, LANES), BF16),
                pltpu.VMEM((4 * ring, ring, size, LANES), BF16),
                pltpu.VMEM((4, ring - 1, ring, size, LANES), BF16),
                pltpu.VMEM((4, ring - 1, size, LANES), BF16),
                pltpu.VMEM((2 * first_half, hidden), BF16),
                pltpu.VMEM((first_half, LANES), F32),
                pltpu.VMEM((size, LANES), F32),
                pltpu.VMEM((2, LANES, hidden), BF16),
                pltpu.VMEM((8, LANES), F32),
                pltpu.VMEM((9, ring, 8, LANES), F32),
                pltpu.VMEM((2 * ring + 1, 16, LANES), F32),
                pltpu.VMEM((2, 16, LANES), F32),
                pltpu.VMEM((ring, 16, LANES), F32),
                pltpu.VMEM((2, 16, LANES), F32),
                dma((4, 2 * ring - 1)), dma((4, 2 * ring - 1)), dma((4, 2 * ring - 1)),
                dma((4, ring - 1, ring)), dma((4, ring - 1, ring)),
                dma((4, ring - 1)), dma((4, ring - 1)),
                dma((2 * ring + 1,)), dma((2 * ring + 1,)),
                dma((ring,)), dma((ring,)),
                dma((2, 4)),
            ],
            compiler_params=pltpu.CompilerParams(collective_id=0, has_side_effects=True, vmem_limit_bytes=52 * 1024 * 1024),
            name="group_exchange",
        )(mix_weight.reshape(1), stats, queries, packed, w_head.T)

    return jax.shard_map(local_step, mesh=mesh, in_specs=(P("data", None), P(None, "model"), P(group_axes, None), P(group_axes), P(), P()), out_specs=P(("data", "store"), "model"), check_vma=False)
```

```python
import functools

import jax
import jax.numpy as jnp
from jax import lax
from jax.experimental import pallas as pl
from jax.experimental.pallas import tpu as pltpu
from jax.sharding import PartitionSpec as P

F32 = jnp.float32
BF16 = jnp.bfloat16
LANES = 128
BATCH = 32
GROUP = 16
PACK_TILES = 32
MESH_ID = pl.DeviceIdType.MESH
ORDER = ((0, 0), (0, 1), (0, 2), (1, 0), (0, 3), (1, 1), (2, 0), (1, 2), (2, 1), (3, 0), (1, 3), (2, 2), (3, 1), (2, 3), (3, 2), (3, 3))


def _scores_kernel(n_blocks, owners, vocab_loc, tok_ref, rtau_ref, q_ref, k_ref, h_ref, stat_ref, hist, vals, top, stage, flag_v, flag_s, word_v, word_s, sem, token_sem):
    step = pl.program_id(0)
    n_core = h_ref.shape[1]
    first_half = h_ref.shape[3]
    block = k_ref.shape[0]
    rows = q_ref.shape[0]
    keys = vals.shape[0] // 2
    filled = 2 * vocab_loc * owners
    batch, n_batches = BATCH, keys // BATCH

    token_copies = [pltpu.make_async_copy(word_v, word_s, token_sem.at[0]), pltpu.make_async_copy(flag_v, flag_s, token_sem.at[1])]

    zero_rows = filled // n_blocks
    hist[pl.ds(pl.multiple_of(step * zero_rows, 8), zero_rows), :] = jnp.zeros((zero_rows, LANES), F32)

    @pl.when(step == 0)
    def _():
        top[...] = jnp.full(top.shape, -jnp.inf, F32)
        rest = hist.shape[0] - filled
        hist[filled:, :] = jnp.zeros((rest, LANES), F32)
        rows_t = [tok_ref[pl.ds(u * n_batches, n_batches)] for u in range(batch)]
        same = jnp.zeros(rows_t[0].shape, jnp.int32)
        for u in range(batch):
            for v in range(u):
                same = jnp.maximum(same, jnp.where(rows_t[u] == rows_t[v], 1, 0))
        flag_v[0, :] = same
        for u in range(batch // 2):
            word_v[0, pl.ds(u * n_batches, n_batches)] = 2 * rows_t[u] | (2 * rows_t[u + batch // 2] << 16)
        for copy in token_copies:
            copy.start()

    sub = min(256, block)
    for part in range(block // sub):
        key = k_ref[part * sub : (part + 1) * sub, :]
        dots = lax.dot_general(key, q_ref[...], (((1,), (1,)), ((), ())), preferred_element_type=F32)
        wide = key.astype(F32)
        norms = jnp.sum(wide * wide, axis=1, keepdims=True)
        score = (2.0 * dots - norms) * rtau_ref[0]
        top[...] = jnp.maximum(top[...], jnp.max(score.reshape(sub // 8, 8, rows), axis=0))
        base = 2 * (step * block + part * sub)
        for half in range(2):
            vals[pl.ds(base + half, sub, stride=2), :] = score[:, half * LANES : (half + 1) * LANES]

    @pl.when(step == n_blocks - 1)
    def _():
        best = jnp.max(top[...], axis=0, keepdims=True)
        pair = jnp.concatenate([best[:, :LANES], best[:, LANES:]], axis=0)
        for copy in token_copies:
            copy.wait()

        def value(u, i):
            return jnp.exp(vals[pl.ds(pl.multiple_of(2 * (u * n_batches + i), 2), 2), :] - pair)

        def spots(i, members):
            out = []
            for u in members:
                word = word_s[0, u * n_batches + i]
                for at in (word & 0xFFFF, lax.shift_right_logical(word, 16)):
                    out.append(pl.ds(pl.multiple_of(at, 2), 2))
            return out, [v for u in members for v in (u, u + batch // 2)]

        def scatter(i, total):
            def distinct():
                sums = []
                for first in range(0, batch // 2, GROUP // 2):
                    at, who = spots(i, range(first, first + GROUP // 2))
                    olds = [hist[p, :] for p in at]
                    adds = [value(u, i) for u in who]
                    for p, old, add in zip(at, olds, adds):
                        hist[p, :] = old + add
                    sums += adds
                while len(sums) > 1:
                    sums = [a + b for a, b in zip(sums[::2], sums[1::2])]
                return sums[0]

            def repeated():
                some = jnp.zeros((2, LANES), F32)
                for first in range(batch // 2):
                    for p, u in zip(*spots(i, [first])):
                        add = value(u, i)
                        hist[p, :] = hist[p, :] + add
                        some = some + add
                return some

            return total + lax.cond(flag_s[0, i] > 0, repeated, distinct)

        total = lax.fori_loop(0, n_batches, scatter, jnp.zeros((2, LANES), F32))
        zeros6 = jnp.zeros((6, LANES), F32)
        stat_ref[...] = jnp.concatenate([pair, zeros6, total, zeros6], axis=0)

        low = lax.broadcasted_iota(jnp.int32, (16, LANES), 1) < LANES // 2
        tiles = PACK_TILES
        copies = []
        for owner in range(owners):
            slot = owner % 2
            if owner >= 2:
                copies[owner - 2].wait()

            def pack(i, _, owner=owner, slot=slot):
                for u in range(tiles):
                    p = pl.multiple_of(i * (16 * tiles) + u * 16, 16)
                    for half in range(2):
                        a = hist[pl.ds(2 * (owner * vocab_loc + p) + half, 16, stride=2), :]
                        b = hist[pl.ds(2 * (owner * vocab_loc + first_half + p) + half, 16, stride=2), :]
                        stage[slot, 2 * half, pl.ds(p, 16), :] = jnp.where(low, a, pltpu.roll(b, 64, axis=1)).astype(BF16)
                        stage[slot, 2 * half + 1, pl.ds(p, 16), :] = jnp.where(low, pltpu.roll(a, 64, axis=1), b).astype(BF16)
                return 0

            lax.fori_loop(0, first_half // (16 * tiles), pack, 0)
            copy = pltpu.make_async_copy(stage.at[slot], h_ref.at[owner // n_core, owner % n_core], sem.at[slot])
            copy.start()
            copies.append(copy)
        copies[-2].wait()
        copies[-1].wait()


def _exchange_kernel(ring, vocab_loc, lam_ref, stat_hbm, q_ref, h_ref, w_ref, out_ref,
                     own, par, ring1, ring2, wbuf, logit, fin, qpad, stat_ref, lm_top, fs, st_recv, st_buf, lm_recv, lm_buf,
                     own_sem, p_send, p_recv, r1_send, r1_recv, r2_send, r2_recv, st_send, st_rsem, lm_send, lm_rsem, w_sem, in_sem):
    s = lax.axis_index("store")
    m = lax.axis_index("model")
    x = lax.div(m, 2)
    c = lax.rem(m, 2)
    size = own.shape[2]
    first_half = 4 * size
    second_half = vocab_loc - first_half
    partner = {"store": s, "model": 2 * x + 1 - c}

    def along_y(d):
        return {"store": lax.rem(s + d + ring, ring), "model": m}

    def along_x(d):
        return {"store": s, "model": 2 * lax.rem(x + d + ring, ring) + c}

    sends = []

    def remote(src, dst, send_sem, recv_sem, peer):
        copy = pltpu.make_async_remote_copy(src_ref=src, dst_ref=dst, send_sem=send_sem, recv_sem=recv_sem,
                                            device_id=peer, device_id_type=MESH_ID)
        copy.start()
        sends.append(copy)
        return copy

    def direction(st):
        return 1 if st % 2 == 0 else -1

    def block_of(st, k):
        here = s if st < 2 else x
        return lax.rem(here - direction(st) * (k + 1) + 2 * ring, ring)

    def sub_of(st, i):
        here = x if st < 2 else s
        return lax.rem(here - direction(st) * (i + 1) + 2 * ring, ring)

    w_copies = {}

    def start_w(q):
        for half in range(2):
            count = size if half == 0 else min(size, second_half - q * size)
            if count <= 0:
                continue
            at = half * first_half + q * size
            copy = pltpu.make_async_copy(w_ref.at[pl.ds(at, count), :], wbuf.at[pl.ds(at, count), :], w_sem.at[half, q])
            copy.start()
            w_copies[q, half] = copy

    own_copies, par_copies = {}, {}

    def fetch(st, k, sub, sem, mine):
        blk = block_of(st, k)
        slot = st * ring + k
        rows = pl.ds(st * size, size)

        def view(core):
            if sub is None:
                return h_ref.at[:, core, blk, rows, :] if st < 2 else h_ref.at[blk, core, :, rows, :]
            return h_ref.at[sub, core, blk, rows, :] if st < 2 else h_ref.at[blk, core, sub, rows, :]

        def into(ref):
            return ref.at[slot] if sub is None else ref.at[slot, sub]

        if mine:
            own_copies[st, sem] = pltpu.make_async_copy(view(c), into(own), own_sem.at[st, sem])
            own_copies[st, sem].start()
        else:
            par_copies[st, sem] = remote(view(1 - c), into(par), p_send.at[st, sem], p_recv.at[st, sem], partner)

    def fetch_first(mine):
        for i in range(ring):
            for st in range(4):
                fetch(st, 0, sub_of(st, i), i, mine)

    stat_copy = pltpu.make_async_copy(stat_hbm, stat_ref, in_sem.at[0])
    stat_copy.start()
    fetch_first(True)
    my_rows = q_ref.at[pl.ds(pl.multiple_of(s * 64, 64), 64), :]
    q_copies = [pltpu.make_async_copy(my_rows, qpad.at[n, pl.ds(64 * n, 64), :], in_sem.at[1 + n]) for n in range(2)]
    for copy in q_copies:
        copy.start()

    barrier = pltpu.get_barrier_semaphore()
    peers = [partner] + [along_y(d) for d in range(1, ring)] + [along_x(d) for d in range(1, ring)]
    for peer in peers:
        pl.semaphore_signal(barrier, inc=1, device_id=peer, device_id_type=MESH_ID)
    pl.semaphore_wait(barrier, len(peers))

    stat_copy.wait()
    first_stat = remote(stat_ref, st_recv.at[0], st_send.at[0], st_rsem.at[0], partner)
    fetch_first(False)
    for k in range(1, ring):
        start_w(k - 1)
        for st in range(4):
            fetch(st, k, None, ring + k - 1, False)
            fetch(st, k, None, ring + k - 1, True)
    start_w(ring - 1)

    if second_half < first_half:
        wbuf[vocab_loc:, :] = jnp.zeros((2 * first_half - vocab_loc, wbuf.shape[1]), BF16)
    blank = jnp.zeros((64, qpad.shape[2]), BF16)
    qpad[0, 64:128, :] = blank
    qpad[1, 0:64, :] = blank

    def merge(a, b):
        high = jnp.maximum(a[0], b[0])
        return high, a[1] * jnp.exp(a[0] - high) + b[1] * jnp.exp(b[0] - high)

    def load(ref):
        return ref[0:8, :], ref[8:16, :]

    low = lax.broadcasted_iota(jnp.int32, (8, LANES), 1) < LANES // 2

    def spread(who, table):
        for half in range(2):
            row = jnp.broadcast_to(table[half : half + 1, :], (8, LANES))
            turned = pltpu.roll(row, 64, axis=1)
            fs[who, 2 * half] = jnp.where(low, row, turned)
            fs[who, 2 * half + 1] = jnp.where(low, turned, row)

    mine = load(stat_ref)
    first_stat.wait_recv()
    theirs = load(st_recv.at[0])
    knn = {"now": merge(mine, theirs)}
    spread(0, jnp.exp(mine[0] - knn["now"][0]))
    spread(1, jnp.exp(theirs[0] - knn["now"][0]))

    def knn_publish(phase, targets):
        st_buf[phase, 0:8, :] = knn["now"][0]
        st_buf[phase, 8:16, :] = knn["now"][1]
        knn["copies"] = []
        for n, peer in targets:
            knn["copies"].append((n, remote(st_buf.at[phase], st_recv.at[n], st_send.at[n], st_rsem.at[n], peer)))

    def knn_collect():
        for n, copy in knn["copies"]:
            copy.wait_recv()
            if n < 2 * ring - 1:
                knn["now"] = merge(knn["now"], load(st_recv.at[n]))

    side = 2 * ring - 1
    knn_publish(0, [(d, along_y(d)) for d in range(1, ring)] + [(side, along_x(1)), (side + 1, along_x(-1))])

    def knn_group():
        knn_collect()
        high = knn["now"][0]
        spread(2, jnp.exp(mine[0] - high))
        spread(3, jnp.exp(theirs[0] - high))
        spread(4, knn["now"][1])
        for st, n in enumerate((1, ring - 1, side, side + 1)):
            spread(5 + st, jnp.exp(st_recv[n, 0:8, :] - high))

    lam = lam_ref[0]

    ring1_copies, ring2_copies = {}, {}

    def process(st, k, i):
        slot = st * ring + k
        sub = sub_of(st, i)
        band = block_of(st, k) if st < 2 else sub
        if k == 0 or i == 0:
            sem = i if k == 0 else ring + k - 1
            own_copies[st, sem].wait()
            par_copies[st, sem].wait_recv()
        if k > 0:
            ring1_copies[st, k - 1, i].wait_recv()
        last = k == ring - 1
        if last and i > 0:
            ring2_copies[st, i - 1].wait_recv()
        f_own = jnp.concatenate([fs[0 if k == 0 else 2, band]] * 2, axis=0)
        f_par = jnp.concatenate([fs[1 if k == 0 else 3, band]] * 2, axis=0)
        f_ring = jnp.concatenate([fs[5 + st, band]] * 2, axis=0) if k == 1 else None
        unroll = 8 if size % 128 == 0 else 1

        def body(t, _):
            for u in range(unroll):
                here = pl.ds(pl.multiple_of(t * (16 * unroll) + 16 * u, 16), 16)
                value = own[slot, sub, here, :].astype(F32) * f_own + par[slot, sub, here, :].astype(F32) * f_par
                if k > 0:
                    came = ring1[st, k - 1, i, here, :].astype(F32)
                    value = value + (came * f_ring if k == 1 else came)
                if last and i > 0:
                    value = value + ring2[st, i - 1, here, :].astype(F32)
                if last and i == ring - 1:
                    fin[here, :] = value
                else:
                    own[slot, sub, here, :] = value.astype(BF16)
            return 0

        lax.fori_loop(0, size // (16 * unroll), body, 0)
        d = direction(st)
        if not last:
            peer = along_y(d) if st < 2 else along_x(d)
            ring1_copies[st, k, i] = remote(own.at[slot, sub], ring1.at[st, k, i], r1_send.at[st, k, i], r1_recv.at[st, k, i], peer)
        elif i < ring - 1:
            peer = along_x(d) if st < 2 else along_y(d)
            ring2_copies[st, i] = remote(own.at[slot, sub], ring2.at[st, i], r2_send.at[st, i], r2_recv.at[st, i], peer)
        else:
            finish(st)

    def head(q):
        if q == 0:
            for copy in q_copies:
                copy.wait()
        for half in range(2):
            if (q, half) in w_copies:
                w_copies[q, half].wait()
        contract = (((1,), (1,)), ((), ()))
        at = q * size
        part = lax.dot_general(wbuf[at : at + size, :], qpad[0], contract, preferred_element_type=F32)
        part = part + lax.dot_general(wbuf[first_half + at : first_half + at + size, :], qpad[1], contract, preferred_element_type=F32)
        if at + size > second_half:
            row = lax.broadcasted_iota(jnp.int32, (size, LANES), 0) + at
            lane = lax.broadcasted_iota(jnp.int32, (size, LANES), 1)
            part = jnp.where((row >= second_half) & (lane >= LANES // 2), -jnp.inf, part)
        logit[at : at + size, :] = part
        best = jnp.max(part.reshape(size // 8, 8, LANES), axis=0)
        lm_top[...] = best if q == 0 else jnp.maximum(lm_top[...], best)

    lm = {}

    def lm_local():
        best = jnp.max(lm_top[...], axis=0, keepdims=True)
        best = jnp.broadcast_to(best, (8, LANES))
        best = jnp.maximum(best, pltpu.roll(best, 64, axis=1))

        def body(t, total):
            here = pl.ds(pl.multiple_of(t * 64, 64), 64)
            new = jnp.exp(logit[here, :].reshape(8, 8, LANES) - best[None])
            logit[here, :] = new.reshape(64, LANES)
            return total + jnp.sum(new, axis=0)

        total = lax.fori_loop(0, first_half // 64, body, jnp.zeros((8, LANES), F32))
        total = jnp.broadcast_to(jnp.sum(total, axis=0, keepdims=True), (8, LANES))
        total = total + pltpu.roll(total, 64, axis=1)
        lm["mine"] = lm["now"] = (best, total)
        lm_publish(0, [partner])

    def lm_publish(phase, targets):
        lm_buf[phase, 0:8, :] = lm["now"][0]
        lm_buf[phase, 8:16, :] = lm["now"][1]
        lm["copies"] = [remote(lm_buf.at[phase], lm_recv.at[phase + n], lm_send.at[phase + n], lm_rsem.at[phase + n], peer)
                        for n, peer in enumerate(targets)]
        lm["slots"] = [phase + n for n in range(len(targets))]

    def lm_collect():
        for copy, n in zip(lm["copies"], lm["slots"]):
            copy.wait_recv()
            lm["now"] = merge(lm["now"], load(lm_recv.at[n]))

    def finish(st):
        scale = lam / fs[4, s]
        lm_scale = lm["scale"]
        wide = min(LANES, size)
        for b in range(size // wide):
            at = st * size + b * wide
            p_knn = fin[b * wide : (b + 1) * wide, :].reshape(wide // 8, 8, LANES) * scale[None]
            p_lm = logit[at : at + wide, :].reshape(wide // 8, 8, LANES) * lm_scale[None]
            mixed = jnp.log(p_knn + p_lm).reshape(wide, LANES).T
            out_ref[:, at : at + wide] = mixed[0:64, :]
            count = min(wide, second_half - at)
            if count > 0:
                out_ref[:, first_half + at : first_half + at + count] = mixed[64:128, :count]

    for place, (k, i) in enumerate(ORDER):
        for st in range(4):
            process(st, k, i)
        if place == 0:
            knn_collect()
            knn_publish(1, [(ring - 1 + d, along_x(d)) for d in range(1, ring)])
        if place == 2:
            knn_group()
        if place in (3, 4, 6, 7):
            head((3, 4, 6, 7).index(place))
        if place == 8:
            lm_local()
        if place == 10:
            lm_collect()
            lm_publish(1, [along_x(d) for d in range(1, ring)])
        if place == 12:
            lm_collect()
            lm["scale"] = (1.0 - lam) * jnp.exp(lm["mine"][0] - lm["now"][0]) / lm["now"][1]
    for copy in sends:
        copy.wait_send()


def solution(mesh):
    store_devs = mesh.shape["store"]
    model_devs = mesh.shape["model"]
    group_axes = ("store", "model")
    cores = 2
    n_x = model_devs // cores
    ring = store_devs

    def local_step(queries, w_head, store_keys, store_tok, temperature, mix_weight):
        vocab_loc = w_head.shape[1]
        rows, hidden = queries.shape
        rows_loc = rows // store_devs
        keys = store_keys.shape[0]
        first_half = -(-vocab_loc // (2 * 4 * LANES)) * 4 * LANES
        size = first_half // 4
        block = min(1024, keys)
        n_blocks = keys // block
        n_batches = keys // BATCH
        hist_rows = 2 * ((model_devs - 1) * vocab_loc + 2 * first_half)
        assert 2 * vocab_loc * model_devs <= 1 << 16
        any_space = pl.BlockSpec(memory_space=pl.ANY)
        smem = pl.BlockSpec(memory_space=pltpu.SMEM)
        vmem = pl.BlockSpec(memory_space=pltpu.VMEM)
        hbm = pl.BlockSpec(memory_space=pltpu.HBM)
        dma = pltpu.SemaphoreType.DMA

        packed, stats = pl.pallas_call(
            functools.partial(_scores_kernel, n_blocks, model_devs, vocab_loc),
            grid=(n_blocks,),
            out_shape=(jax.ShapeDtypeStruct((n_x, cores, store_devs, first_half, LANES), BF16), jax.ShapeDtypeStruct((16, LANES), F32)),
            in_specs=[
                pl.BlockSpec((keys,), lambda i: (0,)),
                smem,
                pl.BlockSpec((rows, hidden), lambda i: (0, 0)),
                pl.BlockSpec((block, hidden), lambda i: (i, 0)),
            ],
            out_specs=(any_space, pl.BlockSpec((16, LANES), lambda i: (0, 0))),
            scratch_shapes=[
                pltpu.VMEM((hist_rows, LANES), F32),
                pltpu.VMEM((2 * keys, LANES), F32),
                pltpu.VMEM((8, rows), F32),
                pltpu.VMEM((2, store_devs, first_half, LANES), BF16),
                pltpu.VMEM((1, n_batches), jnp.int32),
                pltpu.SMEM((1, n_batches), jnp.int32),
                pltpu.VMEM((1, keys // 2), jnp.int32),
                pltpu.SMEM((1, keys // 2), jnp.int32),
                dma((2,)),
                dma((2,)),
            ],
            compiler_params=pltpu.CompilerParams(vmem_limit_bytes=62 * 1024 * 1024),
            name="local_histogram",
        )(store_tok, (1.0 / temperature).reshape(1), queries, store_keys)

        return pl.pallas_call(
            functools.partial(_exchange_kernel, ring, vocab_loc),
            out_shape=jax.ShapeDtypeStruct((rows_loc, vocab_loc), F32),
            in_specs=[smem, hbm, hbm, hbm, hbm],
            out_specs=vmem,
            scratch_shapes=[
                pltpu.VMEM((4 * ring, ring, size, LANES), BF16),
                pltpu.VMEM((4 * ring, ring, size, LANES), BF16),
                pltpu.VMEM((4, ring - 1, ring, size, LANES), BF16),
                pltpu.VMEM((4, ring - 1, size, LANES), BF16),
                pltpu.VMEM((2 * first_half, hidden), BF16),
                pltpu.VMEM((first_half, LANES), F32),
                pltpu.VMEM((size, LANES), F32),
                pltpu.VMEM((2, LANES, hidden), BF16),
                pltpu.VMEM((16, LANES), F32),
                pltpu.VMEM((8, LANES), F32),
                pltpu.VMEM((9, ring, 8, LANES), F32),
                pltpu.VMEM((2 * ring + 1, 16, LANES), F32),
                pltpu.VMEM((2, 16, LANES), F32),
                pltpu.VMEM((ring, 16, LANES), F32),
                pltpu.VMEM((2, 16, LANES), F32),
                dma((4, 2 * ring - 1)), dma((4, 2 * ring - 1)), dma((4, 2 * ring - 1)),
                dma((4, ring - 1, ring)), dma((4, ring - 1, ring)),
                dma((4, ring - 1)), dma((4, ring - 1)),
                dma((2 * ring + 1,)), dma((2 * ring + 1,)),
                dma((ring,)), dma((ring,)),
                dma((2, 4)),
                dma((3,)),
            ],
            compiler_params=pltpu.CompilerParams(collective_id=0, has_side_effects=True, vmem_limit_bytes=52 * 1024 * 1024),
            name="group_exchange",
        )(mix_weight.reshape(1), stats, queries, packed, w_head.T)

    return jax.shard_map(local_step, mesh=mesh, in_specs=(P("data", None), P(None, "model"), P(group_axes, None), P(group_axes), P(), P()), out_specs=P(("data", "store"), "model"), check_vma=False)
```

```python
import functools

import jax
import jax.numpy as jnp
from jax import lax
from jax.experimental import pallas as pl
from jax.experimental.pallas import tpu as pltpu
from jax.sharding import PartitionSpec as P

F32 = jnp.float32
BF16 = jnp.bfloat16
LANES = 128
BATCH = 32
GROUP = 16
PACK_TILES = 32
MESH_ID = pl.DeviceIdType.MESH
ORDER = ((0, 0), (0, 1), (0, 2), (1, 0), (0, 3), (1, 1), (2, 0), (1, 2), (2, 1), (3, 0), (1, 3), (2, 2), (3, 1), (2, 3), (3, 2), (3, 3))


def _scores_kernel(n_blocks, owners, vocab_loc, tok_ref, rtau_ref, q_ref, k_hbm, h_ref, stat_ref, kbuf, hist, vals, top, stage, flag_v, flag_s, word_v, word_s, sem, token_sem, k_sem):
    step = pl.program_id(0)
    n_core = h_ref.shape[1]
    first_half = h_ref.shape[3]
    slots, block, _ = kbuf.shape
    rows = q_ref.shape[0]
    keys = vals.shape[0] // 2
    filled = 2 * vocab_loc * owners
    batch, n_batches = BATCH, keys // BATCH

    token_copies = [pltpu.make_async_copy(word_v, word_s, token_sem.at[0]), pltpu.make_async_copy(flag_v, flag_s, token_sem.at[1])]

    zero_rows = filled // n_blocks
    hist[pl.ds(pl.multiple_of(step * zero_rows, 8), zero_rows), :] = jnp.zeros((zero_rows, LANES), F32)

    def key_copy(n):
        slot = lax.rem(n, slots)
        return pltpu.make_async_copy(k_hbm.at[pl.ds(pl.multiple_of(n * block, block), block), :], kbuf.at[slot], k_sem.at[slot])

    @pl.when(step == 0)
    def _():
        for n in range(min(slots - 1, n_blocks)):
            key_copy(n).start()
        top[...] = jnp.full(top.shape, -jnp.inf, F32)
        rest = hist.shape[0] - filled
        hist[filled:, :] = jnp.zeros((rest, LANES), F32)
        rows_t = [tok_ref[pl.ds(u * n_batches, n_batches)] for u in range(batch)]
        same = jnp.zeros(rows_t[0].shape, jnp.int32)
        for u in range(batch):
            for v in range(u):
                same = jnp.maximum(same, jnp.where(rows_t[u] == rows_t[v], 1, 0))
        flag_v[0, :] = same
        for u in range(batch // 2):
            word_v[0, pl.ds(u * n_batches, n_batches)] = 2 * rows_t[u] | (2 * rows_t[u + batch // 2] << 16)
        for copy in token_copies:
            copy.start()

    @pl.when(step + slots - 1 < n_blocks)
    def _():
        key_copy(step + slots - 1).start()

    key_copy(step).wait()
    k_ref = kbuf.at[lax.rem(step, slots)]
    sub = min(256, block)
    for part in range(block // sub):
        key = k_ref[part * sub : (part + 1) * sub, :]
        dots = lax.dot_general(key, q_ref[...], (((1,), (1,)), ((), ())), preferred_element_type=F32)
        wide = key.astype(F32)
        norms = jnp.sum(wide * wide, axis=1, keepdims=True)
        score = (2.0 * dots - norms) * rtau_ref[0]
        top[...] = jnp.maximum(top[...], jnp.max(score.reshape(sub // 8, 8, rows), axis=0))
        base = 2 * (step * block + part * sub)
        for half in range(2):
            vals[pl.ds(base + half, sub, stride=2), :] = score[:, half * LANES : (half + 1) * LANES]

    @pl.when(step == n_blocks - 1)
    def _():
        best = jnp.max(top[...], axis=0, keepdims=True)
        pair = jnp.concatenate([best[:, :LANES], best[:, LANES:]], axis=0)
        for copy in token_copies:
            copy.wait()

        def value(u, i):
            return jnp.exp(vals[pl.ds(pl.multiple_of(2 * (u * n_batches + i), 2), 2), :] - pair)

        def spots(i, members):
            out = []
            for u in members:
                word = word_s[0, u * n_batches + i]
                for at in (word & 0xFFFF, lax.shift_right_logical(word, 16)):
                    out.append(pl.ds(pl.multiple_of(at, 2), 2))
            return out, [v for u in members for v in (u, u + batch // 2)]

        def scatter(i, total):
            def distinct():
                sums = []
                for first in range(0, batch // 2, GROUP // 2):
                    at, who = spots(i, range(first, first + GROUP // 2))
                    olds = [hist[p, :] for p in at]
                    adds = [value(u, i) for u in who]
                    for p, old, add in zip(at, olds, adds):
                        hist[p, :] = old + add
                    sums += adds
                while len(sums) > 1:
                    sums = [a + b for a, b in zip(sums[::2], sums[1::2])]
                return sums[0]

            def repeated():
                some = jnp.zeros((2, LANES), F32)
                for first in range(batch // 2):
                    for p, u in zip(*spots(i, [first])):
                        add = value(u, i)
                        hist[p, :] = hist[p, :] + add
                        some = some + add
                return some

            return total + lax.cond(flag_s[0, i] > 0, repeated, distinct)

        total = lax.fori_loop(0, n_batches, scatter, jnp.zeros((2, LANES), F32))
        zeros6 = jnp.zeros((6, LANES), F32)
        stat_ref[...] = jnp.concatenate([pair, zeros6, total, zeros6], axis=0)

        low = lax.broadcasted_iota(jnp.int32, (16, LANES), 1) < LANES // 2
        tiles = PACK_TILES
        copies = []
        for owner in range(owners):
            slot = owner % 2
            if owner >= 2:
                copies[owner - 2].wait()

            def pack(i, _, owner=owner, slot=slot):
                for u in range(tiles):
                    p = pl.multiple_of(i * (16 * tiles) + u * 16, 16)
                    for half in range(2):
                        a = hist[pl.ds(2 * (owner * vocab_loc + p) + half, 16, stride=2), :]
                        b = hist[pl.ds(2 * (owner * vocab_loc + first_half + p) + half, 16, stride=2), :]
                        stage[slot, 2 * half, pl.ds(p, 16), :] = jnp.where(low, a, pltpu.roll(b, 64, axis=1)).astype(BF16)
                        stage[slot, 2 * half + 1, pl.ds(p, 16), :] = jnp.where(low, pltpu.roll(a, 64, axis=1), b).astype(BF16)
                return 0

            lax.fori_loop(0, first_half // (16 * tiles), pack, 0)
            copy = pltpu.make_async_copy(stage.at[slot], h_ref.at[owner // n_core, owner % n_core], sem.at[slot])
            copy.start()
            copies.append(copy)
        copies[-2].wait()
        copies[-1].wait()


def _exchange_kernel(ring, vocab_loc, lam_ref, stat_hbm, q_ref, h_ref, w_ref, out_ref,
                     own, par, ring1, ring2, wbuf, logit, fin, qpad, stat_ref, lm_top, fs, st_recv, st_buf, lm_recv, lm_buf,
                     own_sem, p_send, p_recv, r1_send, r1_recv, r2_send, r2_recv, st_send, st_rsem, lm_send, lm_rsem, w_sem, in_sem):
    s = lax.axis_index("store")
    m = lax.axis_index("model")
    x = lax.div(m, 2)
    c = lax.rem(m, 2)
    size = own.shape[2]
    first_half = 4 * size
    second_half = vocab_loc - first_half
    partner = {"store": s, "model": 2 * x + 1 - c}

    def along_y(d):
        return {"store": lax.rem(s + d + ring, ring), "model": m}

    def along_x(d):
        return {"store": s, "model": 2 * lax.rem(x + d + ring, ring) + c}

    sends = []

    def remote(src, dst, send_sem, recv_sem, peer):
        copy = pltpu.make_async_remote_copy(src_ref=src, dst_ref=dst, send_sem=send_sem, recv_sem=recv_sem,
                                            device_id=peer, device_id_type=MESH_ID)
        copy.start()
        sends.append(copy)
        return copy

    def direction(st):
        return 1 if st % 2 == 0 else -1

    def block_of(st, k):
        here = s if st < 2 else x
        return lax.rem(here - direction(st) * (k + 1) + 2 * ring, ring)

    def sub_of(st, i):
        here = x if st < 2 else s
        return lax.rem(here - direction(st) * (i + 1) + 2 * ring, ring)

    w_copies = {}

    def start_w(q):
        for half in range(2):
            count = size if half == 0 else min(size, second_half - q * size)
            if count <= 0:
                continue
            at = half * first_half + q * size
            copy = pltpu.make_async_copy(w_ref.at[pl.ds(at, count), :], wbuf.at[pl.ds(at, count), :], w_sem.at[half, q])
            copy.start()
            w_copies[q, half] = copy

    own_copies, par_copies = {}, {}

    def fetch(st, k, sub, sem, mine):
        blk = block_of(st, k)
        slot = st * ring + k
        rows = pl.ds(st * size, size)

        def view(core):
            if sub is None:
                return h_ref.at[:, core, blk, rows, :] if st < 2 else h_ref.at[blk, core, :, rows, :]
            return h_ref.at[sub, core, blk, rows, :] if st < 2 else h_ref.at[blk, core, sub, rows, :]

        def into(ref):
            return ref.at[slot] if sub is None else ref.at[slot, sub]

        if mine:
            own_copies[st, sem] = pltpu.make_async_copy(view(c), into(own), own_sem.at[st, sem])
            own_copies[st, sem].start()
        else:
            par_copies[st, sem] = remote(view(1 - c), into(par), p_send.at[st, sem], p_recv.at[st, sem], partner)

    def fetch_first(mine):
        for i in range(ring):
            for st in range(4):
                fetch(st, 0, sub_of(st, i), i, mine)

    stat_copy = pltpu.make_async_copy(stat_hbm, stat_ref, in_sem.at[0])
    stat_copy.start()
    fetch_first(True)
    my_rows = q_ref.at[pl.ds(pl.multiple_of(s * 64, 64), 64), :]
    q_copies = [pltpu.make_async_copy(my_rows, qpad.at[n, pl.ds(64 * n, 64), :], in_sem.at[1 + n]) for n in range(2)]
    for copy in q_copies:
        copy.start()

    barrier = pltpu.get_barrier_semaphore()
    peers = [partner] + [along_y(d) for d in range(1, ring)] + [along_x(d) for d in range(1, ring)]
    for peer in peers:
        pl.semaphore_signal(barrier, inc=1, device_id=peer, device_id_type=MESH_ID)
    pl.semaphore_wait(barrier, len(peers))

    stat_copy.wait()
    first_stat = remote(stat_ref, st_recv.at[0], st_send.at[0], st_rsem.at[0], partner)
    fetch_first(False)
    for k in range(1, ring):
        start_w(k - 1)
        for st in range(4):
            fetch(st, k, None, ring + k - 1, False)
            fetch(st, k, None, ring + k - 1, True)
    start_w(ring - 1)

    if second_half < first_half:
        wbuf[vocab_loc:, :] = jnp.zeros((2 * first_half - vocab_loc, wbuf.shape[1]), BF16)
    blank = jnp.zeros((64, qpad.shape[2]), BF16)
    qpad[0, 64:128, :] = blank
    qpad[1, 0:64, :] = blank

    def merge(a, b):
        high = jnp.maximum(a[0], b[0])
        return high, a[1] * jnp.exp(a[0] - high) + b[1] * jnp.exp(b[0] - high)

    def load(ref):
        return ref[0:8, :], ref[8:16, :]

    low = lax.broadcasted_iota(jnp.int32, (8, LANES), 1) < LANES // 2

    def spread(who, table):
        for half in range(2):
            row = jnp.broadcast_to(table[half : half + 1, :], (8, LANES))
            turned = pltpu.roll(row, 64, axis=1)
            fs[who, 2 * half] = jnp.where(low, row, turned)
            fs[who, 2 * half + 1] = jnp.where(low, turned, row)

    mine = load(stat_ref)
    first_stat.wait_recv()
    theirs = load(st_recv.at[0])
    knn = {"now": merge(mine, theirs)}
    spread(0, jnp.exp(mine[0] - knn["now"][0]))
    spread(1, jnp.exp(theirs[0] - knn["now"][0]))

    def knn_publish(phase, targets):
        st_buf[phase, 0:8, :] = knn["now"][0]
        st_buf[phase, 8:16, :] = knn["now"][1]
        knn["copies"] = []
        for n, peer in targets:
            knn["copies"].append((n, remote(st_buf.at[phase], st_recv.at[n], st_send.at[n], st_rsem.at[n], peer)))

    def knn_collect():
        for n, copy in knn["copies"]:
            copy.wait_recv()
            if n < 2 * ring - 1:
                knn["now"] = merge(knn["now"], load(st_recv.at[n]))

    side = 2 * ring - 1
    knn_publish(0, [(d, along_y(d)) for d in range(1, ring)] + [(side, along_x(1)), (side + 1, along_x(-1))])

    def knn_group():
        knn_collect()
        high = knn["now"][0]
        spread(2, jnp.exp(mine[0] - high))
        spread(3, jnp.exp(theirs[0] - high))
        spread(4, knn["now"][1])
        for st, n in enumerate((1, ring - 1, side, side + 1)):
            spread(5 + st, jnp.exp(st_recv[n, 0:8, :] - high))

    lam = lam_ref[0]

    ring1_copies, ring2_copies = {}, {}

    def process(st, k, i, h=None):
        lo, count = (0, size) if h is None else (h * (size // 2), size // 2)
        slot = st * ring + k
        sub = sub_of(st, i)
        band = block_of(st, k) if st < 2 else sub
        last = k == ring - 1
        if not h:
            if k == 0 or i == 0:
                sem = i if k == 0 else ring + k - 1
                own_copies[st, sem].wait()
                par_copies[st, sem].wait_recv()
            if k > 0:
                ring1_copies[st, k - 1, i].wait_recv()
        if last and i > 0 and (st, i - 1, h or 0) in ring2_copies:
            ring2_copies[st, i - 1, h or 0].wait_recv()
        f_own = jnp.concatenate([fs[0 if k == 0 else 2, band]] * 2, axis=0)
        f_par = jnp.concatenate([fs[1 if k == 0 else 3, band]] * 2, axis=0)
        f_ring = jnp.concatenate([fs[5 + st, band]] * 2, axis=0) if k == 1 else None
        unroll = 8 if count % 128 == 0 else 1

        def body(t, _):
            for u in range(unroll):
                here = pl.ds(pl.multiple_of(lo + t * (16 * unroll) + 16 * u, 16), 16)
                value = own[slot, sub, here, :].astype(F32) * f_own + par[slot, sub, here, :].astype(F32) * f_par
                if k > 0:
                    came = ring1[st, k - 1, i, here, :].astype(F32)
                    value = value + (came * f_ring if k == 1 else came)
                if last and i > 0:
                    value = value + ring2[st, i - 1, here, :].astype(F32)
                if last and i == ring - 1:
                    fin[here, :] = value
                else:
                    own[slot, sub, here, :] = value.astype(BF16)
            return 0

        lax.fori_loop(0, count // (16 * unroll), body, 0)
        d = direction(st)
        if not last:
            peer = along_y(d) if st < 2 else along_x(d)
            ring1_copies[st, k, i] = remote(own.at[slot, sub], ring1.at[st, k, i], r1_send.at[st, k, i], r1_recv.at[st, k, i], peer)
        elif i < ring - 1:
            peer = along_x(d) if st < 2 else along_y(d)
            rows = pl.ds(lo, count)
            half = h or 0
            ring2_copies[st, i, half] = remote(own.at[slot, sub, rows, :], ring2.at[st, i, rows, :], r2_send.at[st, i, half], r2_recv.at[st, i, half], peer)
        else:
            finish(st, lo, count)

    def head(q):
        if q == 0:
            for copy in q_copies:
                copy.wait()
        for half in range(2):
            if (q, half) in w_copies:
                w_copies[q, half].wait()
        contract = (((1,), (1,)), ((), ()))
        at = q * size
        part = lax.dot_general(wbuf[at : at + size, :], qpad[0], contract, preferred_element_type=F32)
        part = part + lax.dot_general(wbuf[first_half + at : first_half + at + size, :], qpad[1], contract, preferred_element_type=F32)
        if at + size > second_half:
            row = lax.broadcasted_iota(jnp.int32, (size, LANES), 0) + at
            lane = lax.broadcasted_iota(jnp.int32, (size, LANES), 1)
            part = jnp.where((row >= second_half) & (lane >= LANES // 2), -jnp.inf, part)
        logit[at : at + size, :] = part
        best = jnp.max(part.reshape(size // 8, 8, LANES), axis=0)
        lm_top[...] = best if q == 0 else jnp.maximum(lm_top[...], best)

    lm = {}

    def lm_local():
        best = jnp.max(lm_top[...], axis=0, keepdims=True)
        best = jnp.broadcast_to(best, (8, LANES))
        best = jnp.maximum(best, pltpu.roll(best, 64, axis=1))

        def body(t, total):
            here = pl.ds(pl.multiple_of(t * 64, 64), 64)
            new = jnp.exp(logit[here, :].reshape(8, 8, LANES) - best[None])
            logit[here, :] = new.reshape(64, LANES)
            return total + jnp.sum(new, axis=0)

        total = lax.fori_loop(0, first_half // 64, body, jnp.zeros((8, LANES), F32))
        total = jnp.broadcast_to(jnp.sum(total, axis=0, keepdims=True), (8, LANES))
        total = total + pltpu.roll(total, 64, axis=1)
        lm["mine"] = lm["now"] = (best, total)
        lm_publish(0, [partner])

    def lm_publish(phase, targets):
        lm_buf[phase, 0:8, :] = lm["now"][0]
        lm_buf[phase, 8:16, :] = lm["now"][1]
        lm["copies"] = [remote(lm_buf.at[phase], lm_recv.at[phase + n], lm_send.at[phase + n], lm_rsem.at[phase + n], peer)
                        for n, peer in enumerate(targets)]
        lm["slots"] = [phase + n for n in range(len(targets))]

    def lm_collect():
        for copy, n in zip(lm["copies"], lm["slots"]):
            copy.wait_recv()
            lm["now"] = merge(lm["now"], load(lm_recv.at[n]))

    def finish(st, lo, rows):
        scale = lam / fs[4, s]
        lm_scale = lm["scale"]
        wide = min(LANES, rows)
        for b in range(lo // wide, (lo + rows) // wide):
            at = st * size + b * wide
            p_knn = fin[b * wide : (b + 1) * wide, :].reshape(wide // 8, 8, LANES) * scale[None]
            p_lm = logit[at : at + wide, :].reshape(wide // 8, 8, LANES) * lm_scale[None]
            mixed = jnp.log(p_knn + p_lm).reshape(wide, LANES).T
            out_ref[:, at : at + wide] = mixed[0:64, :]
            count = min(wide, second_half - at)
            if count > 0:
                out_ref[:, first_half + at : first_half + at + count] = mixed[64:128, :count]

    for place, (k, i) in enumerate(ORDER):
        for h in (0, 1) if k == ring - 1 and i > 0 else (None,):
            for st in range(4):
                process(st, k, i, h)
        if place == 0:
            knn_collect()
            knn_publish(1, [(ring - 1 + d, along_x(d)) for d in range(1, ring)])
        if place == 2:
            knn_group()
        if place in (3, 4, 6, 7):
            head((3, 4, 6, 7).index(place))
        if place == 8:
            lm_local()
        if place == 10:
            lm_collect()
            lm_publish(1, [along_x(d) for d in range(1, ring)])
        if place == 12:
            lm_collect()
            lm["scale"] = (1.0 - lam) * jnp.exp(lm["mine"][0] - lm["now"][0]) / lm["now"][1]
    for copy in sends:
        copy.wait_send()


def solution(mesh):
    store_devs = mesh.shape["store"]
    model_devs = mesh.shape["model"]
    group_axes = ("store", "model")
    cores = 2
    n_x = model_devs // cores
    ring = store_devs

    def local_step(queries, w_head, store_keys, store_tok, temperature, mix_weight):
        vocab_loc = w_head.shape[1]
        rows, hidden = queries.shape
        rows_loc = rows // store_devs
        keys = store_keys.shape[0]
        first_half = -(-vocab_loc // (2 * 4 * LANES)) * 4 * LANES
        size = first_half // 4
        block = min(512, keys)
        n_blocks = keys // block
        n_batches = keys // BATCH
        hist_rows = 2 * ((model_devs - 1) * vocab_loc + 2 * first_half)
        assert 2 * vocab_loc * model_devs <= 1 << 16
        any_space = pl.BlockSpec(memory_space=pl.ANY)
        smem = pl.BlockSpec(memory_space=pltpu.SMEM)
        vmem = pl.BlockSpec(memory_space=pltpu.VMEM)
        hbm = pl.BlockSpec(memory_space=pltpu.HBM)
        dma = pltpu.SemaphoreType.DMA

        packed, stats = pl.pallas_call(
            functools.partial(_scores_kernel, n_blocks, model_devs, vocab_loc),
            grid=(n_blocks,),
            out_shape=(jax.ShapeDtypeStruct((n_x, cores, store_devs, first_half, LANES), BF16), jax.ShapeDtypeStruct((16, LANES), F32)),
            in_specs=[
                pl.BlockSpec((keys,), lambda i: (0,)),
                smem,
                pl.BlockSpec((rows, hidden), lambda i: (0, 0)),
                hbm,
            ],
            out_specs=(any_space, pl.BlockSpec((16, LANES), lambda i: (0, 0))),
            scratch_shapes=[
                pltpu.VMEM((4, block, hidden), BF16),
                pltpu.VMEM((hist_rows, LANES), F32),
                pltpu.VMEM((2 * keys, LANES), F32),
                pltpu.VMEM((8, rows), F32),
                pltpu.VMEM((2, store_devs, first_half, LANES), BF16),
                pltpu.VMEM((1, n_batches), jnp.int32),
                pltpu.SMEM((1, n_batches), jnp.int32),
                pltpu.VMEM((1, keys // 2), jnp.int32),
                pltpu.SMEM((1, keys // 2), jnp.int32),
                dma((2,)),
                dma((2,)),
                dma((4,)),
            ],
            compiler_params=pltpu.CompilerParams(vmem_limit_bytes=62 * 1024 * 1024),
            name="local_histogram",
        )(store_tok, (1.0 / temperature).reshape(1), queries, store_keys)

        return pl.pallas_call(
            functools.partial(_exchange_kernel, ring, vocab_loc),
            out_shape=jax.ShapeDtypeStruct((rows_loc, vocab_loc), F32),
            in_specs=[smem, hbm, hbm, hbm, hbm],
            out_specs=vmem,
            scratch_shapes=[
                pltpu.VMEM((4 * ring, ring, size, LANES), BF16),
                pltpu.VMEM((4 * ring, ring, size, LANES), BF16),
                pltpu.VMEM((4, ring - 1, ring, size, LANES), BF16),
                pltpu.VMEM((4, ring - 1, size, LANES), BF16),
                pltpu.VMEM((2 * first_half, hidden), BF16),
                pltpu.VMEM((first_half, LANES), F32),
                pltpu.VMEM((size, LANES), F32),
                pltpu.VMEM((2, LANES, hidden), BF16),
                pltpu.VMEM((16, LANES), F32),
                pltpu.VMEM((8, LANES), F32),
                pltpu.VMEM((9, ring, 8, LANES), F32),
                pltpu.VMEM((2 * ring + 1, 16, LANES), F32),
                pltpu.VMEM((2, 16, LANES), F32),
                pltpu.VMEM((ring, 16, LANES), F32),
                pltpu.VMEM((2, 16, LANES), F32),
                dma((4, 2 * ring - 1)), dma((4, 2 * ring - 1)), dma((4, 2 * ring - 1)),
                dma((4, ring - 1, ring)), dma((4, ring - 1, ring)),
                dma((4, ring - 1, 2)), dma((4, ring - 1, 2)),
                dma((2 * ring + 1,)), dma((2 * ring + 1,)),
                dma((ring,)), dma((ring,)),
                dma((2, 4)),
                dma((3,)),
            ],
            compiler_params=pltpu.CompilerParams(collective_id=0, has_side_effects=True, vmem_limit_bytes=52 * 1024 * 1024),
            name="group_exchange",
        )(mix_weight.reshape(1), stats, queries, packed, w_head.T)

    return jax.shard_map(local_step, mesh=mesh, in_specs=(P("data", None), P(None, "model"), P(group_axes, None), P(group_axes), P(), P()), out_specs=P(("data", "store"), "model"), check_vma=False)
```

```python
import functools

import jax
import jax.numpy as jnp
from jax import lax
from jax.experimental import pallas as pl
from jax.experimental.pallas import tpu as pltpu
from jax.sharding import PartitionSpec as P

F32 = jnp.float32
BF16 = jnp.bfloat16
LANES = 128
BATCH = 32
GROUP = 16
SUB = 256
PACK_TILES = 32
MESH_ID = pl.DeviceIdType.MESH
ORDER = ((0, 0), (0, 1), (0, 2), (1, 0), (0, 3), (1, 1), (2, 0), (1, 2), (2, 1), (3, 0), (1, 3), (2, 2), (3, 1), (2, 3), (3, 2), (3, 3))


def _scores_kernel(n_blocks, owners, vocab_loc, tok_ref, rtau_ref, q_ref, k_hbm, h_ref, stat_ref, kbuf, hist, vals, top, stage, flag_v, flag_s, word_v, word_s, sem, token_sem, k_sem):
    step = pl.program_id(0)
    n_core = h_ref.shape[1]
    first_half = h_ref.shape[3]
    slots, block, _ = kbuf.shape
    rows = q_ref.shape[0]
    keys = vals.shape[0] // 2
    filled = 2 * vocab_loc * owners
    batch, n_batches = BATCH, keys // BATCH

    token_copies = [pltpu.make_async_copy(word_v, word_s, token_sem.at[0]), pltpu.make_async_copy(flag_v, flag_s, token_sem.at[1])]

    zero_rows = filled // n_blocks

    def key_copy(n):
        slot = lax.rem(n, slots)
        return pltpu.make_async_copy(k_hbm.at[pl.ds(pl.multiple_of(n * block, block), block), :], kbuf.at[slot], k_sem.at[slot])

    @pl.when(step == 0)
    def _():
        for n in range(min(slots - 1, n_blocks)):
            key_copy(n).start()
        top[...] = jnp.full(top.shape, -jnp.inf, F32)
        rest = hist.shape[0] - filled
        hist[filled:, :] = jnp.zeros((rest, LANES), F32)
        rows_t = [tok_ref[pl.ds(u * n_batches, n_batches)] for u in range(batch)]
        same = jnp.zeros(rows_t[0].shape, jnp.int32)
        for u in range(batch):
            for v in range(u):
                same = jnp.maximum(same, jnp.where(rows_t[u] == rows_t[v], 1, 0))
        flag_v[0, :] = same
        for u in range(batch // 2):
            word_v[0, pl.ds(u * n_batches, n_batches)] = 2 * rows_t[u] | (2 * rows_t[u + batch // 2] << 16)
        for copy in token_copies:
            copy.start()

    @pl.when(step + slots - 1 < n_blocks)
    def _():
        key_copy(step + slots - 1).start()

    key_copy(step).wait()
    k_ref = kbuf.at[lax.rem(step, slots)]
    hist[pl.ds(pl.multiple_of(step * zero_rows, 8), zero_rows), :] = jnp.zeros((zero_rows, LANES), F32)
    sub = min(SUB, block)
    for part in range(block // sub):
        key = k_ref[part * sub : (part + 1) * sub, :]
        dots = lax.dot_general(key, q_ref[...], (((1,), (1,)), ((), ())), preferred_element_type=F32)
        wide = key.astype(F32)
        norms = jnp.sum(wide * wide, axis=1, keepdims=True)
        score = (2.0 * dots - norms) * rtau_ref[0]
        top[...] = jnp.maximum(top[...], jnp.max(score.reshape(sub // 8, 8, rows), axis=0))
        base = 2 * (step * block + part * sub)
        for half in range(2):
            vals[pl.ds(base + half, sub, stride=2), :] = score[:, half * LANES : (half + 1) * LANES]

    @pl.when(step == n_blocks - 1)
    def _():
        best = jnp.max(top[...], axis=0, keepdims=True)
        pair = jnp.concatenate([best[:, :LANES], best[:, LANES:]], axis=0)
        for copy in token_copies:
            copy.wait()

        def value(u, i):
            return jnp.exp(vals[pl.ds(pl.multiple_of(2 * (u * n_batches + i), 2), 2), :] - pair)

        def spots(i, members):
            out = []
            for u in members:
                word = word_s[0, u * n_batches + i]
                for at in (word & 0xFFFF, lax.shift_right_logical(word, 16)):
                    out.append(pl.ds(pl.multiple_of(at, 2), 2))
            return out, [v for u in members for v in (u, u + batch // 2)]

        def scatter(i, total):
            def distinct():
                sums = []
                for first in range(0, batch // 2, GROUP // 2):
                    at, who = spots(i, range(first, first + GROUP // 2))
                    olds = [hist[p, :] for p in at]
                    adds = [value(u, i) for u in who]
                    for p, old, add in zip(at, olds, adds):
                        hist[p, :] = old + add
                    sums += adds
                while len(sums) > 1:
                    sums = [a + b for a, b in zip(sums[::2], sums[1::2])]
                return sums[0]

            def repeated():
                some = jnp.zeros((2, LANES), F32)
                for first in range(batch // 2):
                    for p, u in zip(*spots(i, [first])):
                        add = value(u, i)
                        hist[p, :] = hist[p, :] + add
                        some = some + add
                return some

            return total + lax.cond(flag_s[0, i] > 0, repeated, distinct)

        total = lax.fori_loop(0, n_batches, scatter, jnp.zeros((2, LANES), F32))
        zeros6 = jnp.zeros((6, LANES), F32)
        stat_ref[...] = jnp.concatenate([pair, zeros6, total, zeros6], axis=0)

        low = lax.broadcasted_iota(jnp.int32, (16, LANES), 1) < LANES // 2
        tiles = PACK_TILES
        copies = []
        for owner in range(owners):
            slot = owner % 2
            if owner >= 2:
                copies[owner - 2].wait()

            def pack(i, _, owner=owner, slot=slot):
                for u in range(tiles):
                    p = pl.multiple_of(i * (16 * tiles) + u * 16, 16)
                    for half in range(2):
                        a = hist[pl.ds(2 * (owner * vocab_loc + p) + half, 16, stride=2), :]
                        b = hist[pl.ds(2 * (owner * vocab_loc + first_half + p) + half, 16, stride=2), :]
                        stage[slot, 2 * half, pl.ds(p, 16), :] = jnp.where(low, a, pltpu.roll(b, 64, axis=1)).astype(BF16)
                        stage[slot, 2 * half + 1, pl.ds(p, 16), :] = jnp.where(low, pltpu.roll(a, 64, axis=1), b).astype(BF16)
                return 0

            lax.fori_loop(0, first_half // (16 * tiles), pack, 0)
            copy = pltpu.make_async_copy(stage.at[slot], h_ref.at[owner // n_core, owner % n_core], sem.at[slot])
            copy.start()
            copies.append(copy)
        copies[-2].wait()
        copies[-1].wait()


def _exchange_kernel(ring, vocab_loc, lam_ref, stat_hbm, q_ref, h_ref, w_ref, out_ref,
                     own, par, ring1, ring2, wbuf, logit, fin, qpad, stat_ref, lm_top, fs, st_recv, st_buf, lm_recv, lm_buf,
                     own_sem, p_send, p_recv, r1_send, r1_recv, r2_send, r2_recv, st_send, st_rsem, lm_send, lm_rsem, w_sem, in_sem):
    s = lax.axis_index("store")
    m = lax.axis_index("model")
    x = lax.div(m, 2)
    c = lax.rem(m, 2)
    size = own.shape[2]
    first_half = 4 * size
    second_half = vocab_loc - first_half
    partner = {"store": s, "model": 2 * x + 1 - c}

    def along_y(d):
        return {"store": lax.rem(s + d + ring, ring), "model": m}

    def along_x(d):
        return {"store": s, "model": 2 * lax.rem(x + d + ring, ring) + c}

    sends = []

    def remote(src, dst, send_sem, recv_sem, peer):
        copy = pltpu.make_async_remote_copy(src_ref=src, dst_ref=dst, send_sem=send_sem, recv_sem=recv_sem,
                                            device_id=peer, device_id_type=MESH_ID)
        copy.start()
        sends.append(copy)
        return copy

    def direction(st):
        return 1 if st % 2 == 0 else -1

    def block_of(st, k):
        here = s if st < 2 else x
        return lax.rem(here - direction(st) * (k + 1) + 2 * ring, ring)

    def sub_of(st, i):
        here = x if st < 2 else s
        return lax.rem(here - direction(st) * (i + 1) + 2 * ring, ring)

    w_copies = {}

    def start_w(q):
        for half in range(2):
            count = size if half == 0 else min(size, second_half - q * size)
            if count <= 0:
                continue
            at = half * first_half + q * size
            copy = pltpu.make_async_copy(w_ref.at[pl.ds(at, count), :], wbuf.at[pl.ds(at, count), :], w_sem.at[half, q])
            copy.start()
            w_copies[q, half] = copy

    own_copies, par_copies = {}, {}

    def fetch(st, k, sub, sem, mine):
        blk = block_of(st, k)
        slot = st * ring + k
        rows = pl.ds(st * size, size)

        def view(core):
            if sub is None:
                return h_ref.at[:, core, blk, rows, :] if st < 2 else h_ref.at[blk, core, :, rows, :]
            return h_ref.at[sub, core, blk, rows, :] if st < 2 else h_ref.at[blk, core, sub, rows, :]

        def into(ref):
            return ref.at[slot] if sub is None else ref.at[slot, sub]

        if mine:
            own_copies[st, sem] = pltpu.make_async_copy(view(c), into(own), own_sem.at[st, sem])
            own_copies[st, sem].start()
        else:
            par_copies[st, sem] = remote(view(1 - c), into(par), p_send.at[st, sem], p_recv.at[st, sem], partner)

    def fetch_first(mine):
        for i in range(ring):
            for st in range(4):
                fetch(st, 0, sub_of(st, i), i, mine)

    stat_copy = pltpu.make_async_copy(stat_hbm, stat_ref, in_sem.at[0])
    stat_copy.start()
    fetch_first(True)
    my_rows = q_ref.at[pl.ds(pl.multiple_of(s * 64, 64), 64), :]
    q_copies = [pltpu.make_async_copy(my_rows, qpad.at[n, pl.ds(64 * n, 64), :], in_sem.at[1 + n]) for n in range(2)]
    for copy in q_copies:
        copy.start()

    barrier = pltpu.get_barrier_semaphore()
    peers = [partner] + [along_y(d) for d in range(1, ring)] + [along_x(d) for d in range(1, ring)]
    for peer in peers:
        pl.semaphore_signal(barrier, inc=1, device_id=peer, device_id_type=MESH_ID)
    pl.semaphore_wait(barrier, len(peers))

    stat_copy.wait()
    first_stat = remote(stat_ref, st_recv.at[0], st_send.at[0], st_rsem.at[0], partner)
    fetch_first(False)
    for k in range(1, ring):
        start_w(k - 1)
        for st in range(4):
            fetch(st, k, None, ring + k - 1, False)
            fetch(st, k, None, ring + k - 1, True)
    start_w(ring - 1)

    if second_half < first_half:
        wbuf[vocab_loc:, :] = jnp.zeros((2 * first_half - vocab_loc, wbuf.shape[1]), BF16)
    blank = jnp.zeros((64, qpad.shape[2]), BF16)
    qpad[0, 64:128, :] = blank
    qpad[1, 0:64, :] = blank

    def merge(a, b):
        high = jnp.maximum(a[0], b[0])
        return high, a[1] * jnp.exp(a[0] - high) + b[1] * jnp.exp(b[0] - high)

    def load(ref):
        return ref[0:8, :], ref[8:16, :]

    low = lax.broadcasted_iota(jnp.int32, (8, LANES), 1) < LANES // 2

    def spread(who, table):
        for half in range(2):
            row = jnp.broadcast_to(table[half : half + 1, :], (8, LANES))
            turned = pltpu.roll(row, 64, axis=1)
            fs[who, 2 * half] = jnp.where(low, row, turned)
            fs[who, 2 * half + 1] = jnp.where(low, turned, row)

    mine = load(stat_ref)
    first_stat.wait_recv()
    theirs = load(st_recv.at[0])
    knn = {"now": merge(mine, theirs)}
    spread(0, jnp.exp(mine[0] - knn["now"][0]))
    spread(1, jnp.exp(theirs[0] - knn["now"][0]))

    def knn_publish(phase, targets):
        st_buf[phase, 0:8, :] = knn["now"][0]
        st_buf[phase, 8:16, :] = knn["now"][1]
        knn["copies"] = []
        for n, peer in targets:
            knn["copies"].append((n, remote(st_buf.at[phase], st_recv.at[n], st_send.at[n], st_rsem.at[n], peer)))

    def knn_collect():
        for n, copy in knn["copies"]:
            copy.wait_recv()
            if n < 2 * ring - 1:
                knn["now"] = merge(knn["now"], load(st_recv.at[n]))

    side = 2 * ring - 1
    knn_publish(0, [(d, along_y(d)) for d in range(1, ring)] + [(side, along_x(1)), (side + 1, along_x(-1))])

    def knn_group():
        knn_collect()
        high = knn["now"][0]
        spread(2, jnp.exp(mine[0] - high))
        spread(3, jnp.exp(theirs[0] - high))
        spread(4, knn["now"][1])
        for st, n in enumerate((1, ring - 1, side, side + 1)):
            spread(5 + st, jnp.exp(st_recv[n, 0:8, :] - high))

    lam = lam_ref[0]

    ring1_copies, ring2_copies = {}, {}

    def process(st, k, i, h=None):
        lo, count = (0, size) if h is None else (h * (size // 2), size // 2)
        slot = st * ring + k
        sub = sub_of(st, i)
        band = block_of(st, k) if st < 2 else sub
        last = k == ring - 1
        if not h:
            if k == 0 or i == 0:
                sem = i if k == 0 else ring + k - 1
                own_copies[st, sem].wait()
                par_copies[st, sem].wait_recv()
            if k > 0:
                ring1_copies[st, k - 1, i].wait_recv()
        if last and i > 0 and (st, i - 1, h or 0) in ring2_copies:
            ring2_copies[st, i - 1, h or 0].wait_recv()
        f_own = jnp.concatenate([fs[0 if k == 0 else 2, band]] * 2, axis=0)
        f_par = jnp.concatenate([fs[1 if k == 0 else 3, band]] * 2, axis=0)
        f_ring = jnp.concatenate([fs[5 + st, band]] * 2, axis=0) if k == 1 else None
        unroll = 8 if count % 128 == 0 else 1

        def body(t, _):
            for u in range(unroll):
                here = pl.ds(pl.multiple_of(lo + t * (16 * unroll) + 16 * u, 16), 16)
                value = own[slot, sub, here, :].astype(F32) * f_own + par[slot, sub, here, :].astype(F32) * f_par
                if k > 0:
                    came = ring1[st, k - 1, i, here, :].astype(F32)
                    value = value + (came * f_ring if k == 1 else came)
                if last and i > 0:
                    value = value + ring2[st, i - 1, here, :].astype(F32)
                if last and i == ring - 1:
                    fin[here, :] = value
                else:
                    own[slot, sub, here, :] = value.astype(BF16)
            return 0

        lax.fori_loop(0, count // (16 * unroll), body, 0)
        d = direction(st)
        if not last:
            peer = along_y(d) if st < 2 else along_x(d)
            ring1_copies[st, k, i] = remote(own.at[slot, sub], ring1.at[st, k, i], r1_send.at[st, k, i], r1_recv.at[st, k, i], peer)
        elif i < ring - 1:
            peer = along_x(d) if st < 2 else along_y(d)
            rows = pl.ds(lo, count)
            half = h or 0
            ring2_copies[st, i, half] = remote(own.at[slot, sub, rows, :], ring2.at[st, i, rows, :], r2_send.at[st, i, half], r2_recv.at[st, i, half], peer)
        else:
            finish(st, lo, count)

    def head(q):
        if q == 0:
            for copy in q_copies:
                copy.wait()
        for half in range(2):
            if (q, half) in w_copies:
                w_copies[q, half].wait()
        contract = (((1,), (1,)), ((), ()))
        at = q * size
        part = lax.dot_general(wbuf[at : at + size, :], qpad[0], contract, preferred_element_type=F32)
        part = part + lax.dot_general(wbuf[first_half + at : first_half + at + size, :], qpad[1], contract, preferred_element_type=F32)
        if at + size > second_half:
            row = lax.broadcasted_iota(jnp.int32, (size, LANES), 0) + at
            lane = lax.broadcasted_iota(jnp.int32, (size, LANES), 1)
            part = jnp.where((row >= second_half) & (lane >= LANES // 2), -jnp.inf, part)
        logit[at : at + size, :] = part
        best = jnp.max(part.reshape(size // 8, 8, LANES), axis=0)
        lm_top[...] = best if q == 0 else jnp.maximum(lm_top[...], best)

    lm = {}

    def lm_local():
        best = jnp.max(lm_top[...], axis=0, keepdims=True)
        best = jnp.broadcast_to(best, (8, LANES))
        best = jnp.maximum(best, pltpu.roll(best, 64, axis=1))

        def body(t, total):
            here = pl.ds(pl.multiple_of(t * 64, 64), 64)
            new = jnp.exp(logit[here, :].reshape(8, 8, LANES) - best[None])
            logit[here, :] = new.reshape(64, LANES)
            return total + jnp.sum(new, axis=0)

        total = lax.fori_loop(0, first_half // 64, body, jnp.zeros((8, LANES), F32))
        total = jnp.broadcast_to(jnp.sum(total, axis=0, keepdims=True), (8, LANES))
        total = total + pltpu.roll(total, 64, axis=1)
        lm["mine"] = lm["now"] = (best, total)
        lm_publish(0, [partner])

    def lm_publish(phase, targets):
        lm_buf[phase, 0:8, :] = lm["now"][0]
        lm_buf[phase, 8:16, :] = lm["now"][1]
        lm["copies"] = [remote(lm_buf.at[phase], lm_recv.at[phase + n], lm_send.at[phase + n], lm_rsem.at[phase + n], peer)
                        for n, peer in enumerate(targets)]
        lm["slots"] = [phase + n for n in range(len(targets))]

    def lm_collect():
        for copy, n in zip(lm["copies"], lm["slots"]):
            copy.wait_recv()
            lm["now"] = merge(lm["now"], load(lm_recv.at[n]))

    def finish(st, lo, rows):
        scale = lam / fs[4, s]
        lm_scale = lm["scale"]
        wide = min(LANES, rows)
        for b in range(lo // wide, (lo + rows) // wide):
            at = st * size + b * wide
            p_knn = fin[b * wide : (b + 1) * wide, :].reshape(wide // 8, 8, LANES) * scale[None]
            p_lm = logit[at : at + wide, :].reshape(wide // 8, 8, LANES) * lm_scale[None]
            mixed = jnp.log(p_knn + p_lm).reshape(wide, LANES).T
            out_ref[:, at : at + wide] = mixed[0:64, :]
            count = min(wide, second_half - at)
            if count > 0:
                out_ref[:, first_half + at : first_half + at + count] = mixed[64:128, :count]

    for place, (k, i) in enumerate(ORDER):
        for h in (0, 1) if k == ring - 1 and i > 0 else (None,):
            for st in range(4):
                process(st, k, i, h)
        if place == 0:
            knn_collect()
            knn_publish(1, [(ring - 1 + d, along_x(d)) for d in range(1, ring)])
        if place == 2:
            knn_group()
        if place in (3, 4, 6, 7):
            head((3, 4, 6, 7).index(place))
        if place == 8:
            lm_local()
        if place == 10:
            lm_collect()
            lm_publish(1, [along_x(d) for d in range(1, ring)])
        if place == 12:
            lm_collect()
            lm["scale"] = (1.0 - lam) * jnp.exp(lm["mine"][0] - lm["now"][0]) / lm["now"][1]
    for copy in sends:
        copy.wait_send()


def solution(mesh):
    store_devs = mesh.shape["store"]
    model_devs = mesh.shape["model"]
    group_axes = ("store", "model")
    cores = 2
    n_x = model_devs // cores
    ring = store_devs

    def local_step(queries, w_head, store_keys, store_tok, temperature, mix_weight):
        vocab_loc = w_head.shape[1]
        rows, hidden = queries.shape
        rows_loc = rows // store_devs
        keys = store_keys.shape[0]
        first_half = -(-vocab_loc // (2 * 4 * LANES)) * 4 * LANES
        size = first_half // 4
        block = min(1024, keys)
        n_blocks = keys // block
        n_batches = keys // BATCH
        hist_rows = 2 * ((model_devs - 1) * vocab_loc + 2 * first_half)
        assert 2 * vocab_loc * model_devs <= 1 << 16
        any_space = pl.BlockSpec(memory_space=pl.ANY)
        smem = pl.BlockSpec(memory_space=pltpu.SMEM)
        vmem = pl.BlockSpec(memory_space=pltpu.VMEM)
        hbm = pl.BlockSpec(memory_space=pltpu.HBM)
        dma = pltpu.SemaphoreType.DMA

        packed, stats = pl.pallas_call(
            functools.partial(_scores_kernel, n_blocks, model_devs, vocab_loc),
            grid=(n_blocks,),
            out_shape=(jax.ShapeDtypeStruct((n_x, cores, store_devs, first_half, LANES), BF16), jax.ShapeDtypeStruct((16, LANES), F32)),
            in_specs=[
                pl.BlockSpec((keys,), lambda i: (0,)),
                smem,
                pl.BlockSpec((rows, hidden), lambda i: (0, 0)),
                hbm,
            ],
            out_specs=(any_space, pl.BlockSpec((16, LANES), lambda i: (0, 0))),
            scratch_shapes=[
                pltpu.VMEM((3, block, hidden), BF16),
                pltpu.VMEM((hist_rows, LANES), F32),
                pltpu.VMEM((2 * keys, LANES), F32),
                pltpu.VMEM((8, rows), F32),
                pltpu.VMEM((2, store_devs, first_half, LANES), BF16),
                pltpu.VMEM((1, n_batches), jnp.int32),
                pltpu.SMEM((1, n_batches), jnp.int32),
                pltpu.VMEM((1, keys // 2), jnp.int32),
                pltpu.SMEM((1, keys // 2), jnp.int32),
                dma((2,)),
                dma((2,)),
                dma((3,)),
            ],
            compiler_params=pltpu.CompilerParams(vmem_limit_bytes=62 * 1024 * 1024),
            name="local_histogram",
        )(store_tok, (1.0 / temperature).reshape(1), queries, store_keys)

        return pl.pallas_call(
            functools.partial(_exchange_kernel, ring, vocab_loc),
            out_shape=jax.ShapeDtypeStruct((rows_loc, vocab_loc), F32),
            in_specs=[smem, hbm, hbm, hbm, hbm],
            out_specs=vmem,
            scratch_shapes=[
                pltpu.VMEM((4 * ring, ring, size, LANES), BF16),
                pltpu.VMEM((4 * ring, ring, size, LANES), BF16),
                pltpu.VMEM((4, ring - 1, ring, size, LANES), BF16),
                pltpu.VMEM((4, ring - 1, size, LANES), BF16),
                pltpu.VMEM((2 * first_half, hidden), BF16),
                pltpu.VMEM((first_half, LANES), F32),
                pltpu.VMEM((size, LANES), F32),
                pltpu.VMEM((2, LANES, hidden), BF16),
                pltpu.VMEM((16, LANES), F32),
                pltpu.VMEM((8, LANES), F32),
                pltpu.VMEM((9, ring, 8, LANES), F32),
                pltpu.VMEM((2 * ring + 1, 16, LANES), F32),
                pltpu.VMEM((2, 16, LANES), F32),
                pltpu.VMEM((ring, 16, LANES), F32),
                pltpu.VMEM((2, 16, LANES), F32),
                dma((4, 2 * ring - 1)), dma((4, 2 * ring - 1)), dma((4, 2 * ring - 1)),
                dma((4, ring - 1, ring)), dma((4, ring - 1, ring)),
                dma((4, ring - 1, 2)), dma((4, ring - 1, 2)),
                dma((2 * ring + 1,)), dma((2 * ring + 1,)),
                dma((ring,)), dma((ring,)),
                dma((2, 4)),
                dma((3,)),
            ],
            compiler_params=pltpu.CompilerParams(collective_id=0, has_side_effects=True, vmem_limit_bytes=52 * 1024 * 1024),
            name="group_exchange",
        )(mix_weight.reshape(1), stats, queries, packed, w_head.T)

    return jax.shard_map(local_step, mesh=mesh, in_specs=(P("data", None), P(None, "model"), P(group_axes, None), P(group_axes), P(), P()), out_specs=P(("data", "store"), "model"), check_vma=False)
```
